32 devices in a mesh: dp: 4 (over y, core), seq: 8 (over z, x).
Axes of the slice: x: 2, y: 2, z: 4, core: 2. Of those that a mesh axis runs over, the one named last changes fastest.
Arguments:
- queries: bfloat16 [4, 1024, 2048], P('dp', 'seq'), may hold values from -12 to 12
- keys: bfloat16 [4, 1024, 512], P('dp', 'seq'), may hold values from -4 to 4
- values: bfloat16 [4, 1024, 512], P('dp', 'seq'), may hold values from -6 to 6
- segments: int32 [4, 1024], P('dp', 'seq'), may hold values from 0 to 3, never falling along the last dimension, each value on 1 to 896 neighbouring positions
- task_ids: int32 [4], replicated, may hold values from 0 to 15
- prompt_keys: bfloat16 [16, 128, 512], P('seq'), may hold values from -4 to 4
- prompt_values: bfloat16 [16, 128, 512], P('seq'), may hold values from -6 to 6
- grad_out: bfloat16 [4, 1024, 2048], P('dp', 'seq'), may hold values from -6 to 6
Outputs:
- attended: bfloat16 [4, 1024, 2048], P('dp', 'seq')
- prompt_key_grad: float32 [16, 128, 512], P('seq')
- prompt_value_grad: float32 [16, 128, 512], P('seq')
The draws below stay inside these ranges and needn't reach their ends.
Inputs may be any that keep to these rules, and one draw needn't show every extreme that they name: `segments`: along each example the document numbers never fall; one document holds 896 tokens.
All inputs are finite; a program needn't handle non-finite values.
Results may differ from the reference program's by a relative error of at most 0.0096.
Values may be sent and summed in bfloat16 or wider, within the bound.
A program may use at most 128 MiB of HBM per device.

```python
import math
import jax
import jax.numpy as jnp
import numpy as np
from jax import lax

KVH = 4
GROUP = 4
HD = 128
PROMPT = 128
DOCS = 4
HEADS = 16
TOKENS = 1024
TASKS = 16
BATCH = 4
LONGEST = 896


def draw_queries(key, part):
    base_key = jax.random.fold_in(key, 7)
    shape = (BATCH, TOKENS, KVH * GROUP * HD)
    field = jnp.clip(3.0 * jax.random.normal(base_key, shape, jnp.float32), -12.0, 12.0)
    return field.astype(jnp.bfloat16)


def draw_prompt_keys(key, part):
    base_key = jax.random.fold_in(key, 11)
    shape = (TASKS, PROMPT, KVH * HD)
    field = jnp.clip(jax.random.normal(base_key, shape, jnp.float32), -4.0, 4.0)
    return field.astype(jnp.bfloat16)


def with_ends(result, stream_key, smallest, top_value):
    longest = result.shape.index(max(result.shape))
    spots = []
    for shift in (0, 1):
        where = [jax.random.randint(jax.random.fold_in(stream_key, axis), (), 0, length) for axis, length in enumerate(result.shape)]
        where[longest] = (where[longest] + shift) % result.shape[longest]
        spots.append(tuple(where))
    return result.at[spots[0]].set(smallest).at[spots[1]].set(top_value)


def block_levels(key, extent, shards, least, high):
    level = 1.0
    for dim, shards_of in shards:
        draws = jax.random.uniform(jax.random.fold_in(jax.random.fold_in(key, 6), dim), (shards_of,), jnp.float32, least / len(shards), high / len(shards))
        level = level * jnp.repeat(jnp.exp(draws), extent[dim] // shards_of).reshape((-1,) + (1,) * (len(extent) - 1 - dim))
    return level


def split_up(count, total, bound, skew):
    weights = [(1 << 20) // math.isqrt(rank ** skew) + 1 for rank in range(2, count + 1)]
    spare, given = total - bound - (count - 1), [1] * (count - 1)
    while spare > 0:
        candidates = [i for i in range(count - 1) if given[i] < bound]
        mass, left = sum([weights[i] for i in candidates]), spare
        for i in candidates:
            more = min(bound - given[i], max(1, left * weights[i] // mass), spare)
            given[i] = given[i] + more
            spare = spare - more
    return np.array([bound] + given)


def uneven_parts(key, number_of, total, limit, skew):
    if number_of == 2:
        one = jax.random.randint(key, (), max(1, total - limit), min(limit, total - 1) + 1)
        return jnp.stack([one, total - one])
    lengths = jnp.asarray(split_up(number_of, total, limit, skew), jnp.int32)
    couples = (number_of - 1) // 2
    giver, taker = lengths[1:1 + 2 * couples:2], lengths[2:2 + 2 * couples:2]
    slack = jnp.minimum(giver - 1, limit - taker)
    moved = jax.random.randint(jax.random.fold_in(key, 1), (couples,), 0, 1 << 20) % (slack + 1)
    lengths = lengths.at[1:1 + 2 * couples:2].set(giver - moved).at[2:2 + 2 * couples:2].set(taker + moved)
    return lengths[jax.random.permutation(jax.random.fold_in(key, 2), number_of)]


def noise(own_key, shape, width, most, shards=(), kind=jnp.bfloat16):
    result = jax.random.normal(own_key, shape, jnp.float32) * width
    if len(shards) > 0:
        result = block_levels(own_key, shape, shards, -0.22, 0.18) * result
    return jnp.clip(result, min=-most, max=most).astype(kind)


def setup_inputs(seed: int = 0) -> dict:
    arg_keys = jax.random.split(jax.random.key(seed), 9)
    queries = draw_queries(jax.random.fold_in(arg_keys[8], 71), 0)
    keys = noise(arg_keys[1], (BATCH, TOKENS, KVH * HD), 1.0, 4.0, ((0, 4), (1, 8)))
    values = noise(arg_keys[2], (BATCH, TOKENS, KVH * HD), 1.0, 6.0, ((0, 4), (1, 8)))
    segments = jax.vmap(lambda own: jnp.searchsorted(jnp.cumsum(uneven_parts(own, DOCS, TOKENS, LONGEST, 2)), jnp.arange(TOKENS), side="right"))(jax.random.split(arg_keys[3], BATCH)).reshape((BATCH, TOKENS)).astype(jnp.int32)
    task_ids = with_ends(jax.random.randint(arg_keys[4], (BATCH,), 0, TASKS), jax.random.fold_in(arg_keys[4], 1), 0, TASKS - 1).astype(jnp.int32)
    prompt_keys = draw_prompt_keys(jax.random.fold_in(arg_keys[8], 71), 0)
    prompt_values = noise(arg_keys[6], (TASKS, PROMPT, KVH * HD), 1.0, 6.0, ((0, 8),))
    grad_out = noise(arg_keys[7], (BATCH, TOKENS, HEADS * HD), 1.0, 6.0, ((0, 4), (1, 8)))
    return dict(queries=queries, keys=keys, values=values, segments=segments, task_ids=task_ids, prompt_keys=prompt_keys, prompt_values=prompt_values, grad_out=grad_out)


def rounded(tensor):
    return lax.optimization_barrier(tensor.astype(jnp.bfloat16)).astype(jnp.float32)

def one_example(query_rows, key_rows, value_rows, segment_row, grad_rows, chosen_keys, chosen_values):
    tokens_all = query_rows.shape[0]
    block_rows = math.gcd(tokens_all, 256)
    block_count = tokens_all // block_rows
    scaling = 1.0 / math.sqrt(HD)
    key_heads = key_rows.reshape(tokens_all, KVH, HD).astype(jnp.float32)
    value_heads = value_rows.reshape(tokens_all, KVH, HD).astype(jnp.float32)
    prompt_key_heads = chosen_keys.reshape(PROMPT, KVH, HD).astype(jnp.float32)
    prompt_value_heads = chosen_values.reshape(PROMPT, KVH, HD).astype(jnp.float32)
    key_index = lax.iota(jnp.int32, tokens_all)

    def per_block(carried, block_index):
        first_row = (block_index * block_rows).astype(jnp.int32)
        query_heads = lax.dynamic_slice_in_dim(query_rows, first_row, block_rows, 0)
        query_heads = query_heads.reshape(block_rows, KVH, GROUP, HD).astype(jnp.float32)
        grad_heads = lax.dynamic_slice_in_dim(grad_rows, first_row, block_rows, 0)
        grad_heads = grad_heads.reshape(block_rows, KVH, GROUP, HD).astype(jnp.float32)
        query_segments = lax.dynamic_slice_in_dim(segment_row, first_row, block_rows, 0)
        query_index = first_row + lax.iota(jnp.int32, block_rows)
        visible = (segment_row[None, :] == query_segments[:, None]) & (key_index[None, :] <= query_index[:, None])
        mask_wide = visible[:, None, None, :]
        scores = jnp.einsum('tkgd,skd->tkgs', query_heads, key_heads) * scaling
        prompt_scores = jnp.einsum('tkgd,pkd->tkgp', query_heads, prompt_key_heads) * scaling
        new_peak = jnp.maximum(lax.optimization_barrier(jnp.max(jnp.where(mask_wide, scores, -jnp.inf), axis=-1)), lax.optimization_barrier(jnp.max(prompt_scores, axis=-1)))
        weights = jnp.where(mask_wide, jnp.exp(scores - new_peak[..., None]), 0.0)
        prompt_weights = jnp.exp(prompt_scores - new_peak[..., None])
        totals = lax.optimization_barrier(jnp.sum(weights, axis=-1)) + lax.optimization_barrier(jnp.sum(prompt_weights, axis=-1))
        accumulated = jnp.einsum('tkgs,skd->tkgd', rounded(weights), value_heads)
        accumulated = accumulated + jnp.einsum('tkgp,pkd->tkgd', rounded(prompt_weights), prompt_value_heads)
        attended = (accumulated / totals[..., None]).astype(jnp.bfloat16)
        log_norm = new_peak + jnp.log(totals)
        attended_wide = lax.optimization_barrier(attended).astype(jnp.float32)
        row_delta = lax.optimization_barrier(jnp.sum(grad_heads * attended_wide, axis=-1))
        prompt_probs = jnp.exp(prompt_scores - log_norm[..., None])
        prompt_dots = jnp.einsum('tkgd,pkd->tkgp', grad_heads, prompt_value_heads)
        score_grad = prompt_probs * (prompt_dots - row_delta[..., None])
        value_part = jnp.einsum('tkgp,tkgd->pkd', rounded(prompt_probs), grad_heads)
        key_part = jnp.einsum('tkgp,tkgd->pkd', rounded(score_grad), query_heads) * scaling
        return ((carried[0] + key_part, carried[1] + value_part), attended.reshape(block_rows, KVH * GROUP * HD))
    zeros = jnp.zeros((PROMPT, KVH, HD), jnp.float32)
    sums, pieces = lax.scan(per_block, (zeros, zeros), jnp.arange(block_count, dtype=jnp.int32))
    attended_all = pieces.reshape(tokens_all, KVH * GROUP * HD)
    return (attended_all, sums[0].reshape(PROMPT, KVH * HD), sums[1].reshape(PROMPT, KVH * HD))

def reference(queries, keys, values, segments, task_ids, prompt_keys, prompt_values, grad_out):
    outputs = []
    key_grad = jnp.zeros((TASKS, PROMPT, KVH * HD), jnp.float32)
    value_grad = jnp.zeros((TASKS, PROMPT, KVH * HD), jnp.float32)
    task_range = lax.iota(jnp.int32, TASKS)
    for example in range(queries.shape[0]):
        task_now = task_ids[example].astype(jnp.int32)
        chosen_keys = lax.dynamic_index_in_dim(prompt_keys, task_now, 0, keepdims=False)
        chosen_values = lax.dynamic_index_in_dim(prompt_values, task_now, 0, keepdims=False)
        attended, key_part, value_part = one_example(queries[example], keys[example], values[example], segments[example], grad_out[example], chosen_keys, chosen_values)
        outputs.append(attended)
        chosen = (task_range == task_now)[:, None, None]
        key_grad = key_grad + jnp.where(chosen, key_part[None], 0.0)
        value_grad = value_grad + jnp.where(chosen, value_part[None], 0.0)
    return (jnp.stack(outputs), key_grad, value_grad)
```

```python
import functools
import math

import jax
import jax.numpy as jnp
from jax import lax
from jax.experimental import pallas as pl
from jax.experimental.pallas import tpu as pltpu
from jax.sharding import PartitionSpec as P

KVH = 4
GROUP = 4
HD = 128
PROMPT = 128
SLOTS = 2 * KVH


def dot_nt(a, b):
    return lax.dot_general(a, b, (((1,), (1,)), ((), ())), preferred_element_type=jnp.float32)


def dot_tn(a, b):
    return lax.dot_general(a, b, (((0,), (0,)), ((), ())), preferred_element_type=jnp.float32)


def dot_nn(a, b):
    return lax.dot_general(a, b, (((1,), (0,)), ((), ())), preferred_element_type=jnp.float32)


def head_cols(c):
    return slice(c * HD, (c + 1) * HD)


def kernel(
    n, n_dp, task_ref, q_ref, k_ref, v_ref, seg_ref, pk_ref, pv_ref, g_ref,
    att_ref, kg_ref, vg_ref,
    kv, segs, sel, prs, pp, part, grs, gath, m_ref, l_ref, acc_ref,
    seg_s, seg_r, prs_s, prs_r, pag_s, pag_r, z_s, z_r, x_s, x_r,
    grs_s, grs_r, gag_s, gag_r, y_s, y_r, c_s, c_r,
):
    tok = q_ref.shape[0]
    bank = pk_ref.shape[0]
    rows = SLOTS * PROMPT // n
    n_hi = n // 2
    n_dh = n_dp // 2
    scale = 1.0 / math.sqrt(HD)
    me = lax.axis_index("seq")
    dp = lax.axis_index("dp")
    hi, lo = me // 2, me % 2
    dh, dl = dp // 2, dp % 2

    def remote(src, dst, s_sem, r_sem, to_dp, to_seq):
        return pltpu.make_async_remote_copy(
            src_ref=src, dst_ref=dst, send_sem=s_sem, recv_sem=r_sem,
            device_id=(to_dp, to_seq), device_id_type=pl.DeviceIdType.MESH,
        )

    def other(d, base, count):
        return lax.rem(base + d, count)

    def chunk(ref, j):
        return ref.at[pl.ds(pl.multiple_of(j * rows, rows), rows)]

    barrier = pltpu.get_barrier_semaphore()

    @pl.loop(1, n)
    def _(d):
        pl.semaphore_signal(barrier, inc=1, device_id=(dp, other(d, me, n)),
                            device_id_type=pl.DeviceIdType.MESH)

    @pl.loop(1, n_dp)
    def _(d):
        pl.semaphore_signal(barrier, inc=1, device_id=(other(d, dp, n_dp), me),
                            device_id_type=pl.DeviceIdType.MESH)

    task = task_ref[dp]
    for s in range(SLOTS):
        src = pk_ref if s < KVH else pv_ref
        total = jnp.zeros((PROMPT, HD), jnp.bfloat16)
        for k in range(bank):
            hit = jnp.full((PROMPT, HD), task, jnp.int32) == me * bank + k
            total = jnp.where(hit, src[k, :, head_cols(s % KVH)], total)
        sel[s * PROMPT:(s + 1) * PROMPT, :] = total

    pl.semaphore_wait(barrier, n - 1 + n_dp - 1)

    def seg_copy(src_rank, dst_rank):
        return remote(seg_ref, segs.at[src_rank], seg_s.at[dst_rank], seg_r.at[src_rank], dp, dst_rank)

    def prs_copy(src_rank, dst_rank):
        return remote(chunk(sel, dst_rank), prs.at[src_rank], prs_s.at[dst_rank], prs_r.at[src_rank], dp, dst_rank)

    def pag_copy(src_rank, dst_rank):
        return remote(chunk(pp, src_rank), chunk(pp, src_rank), pag_s.at[dst_rank], pag_r.at[src_rank], dp, dst_rank)

    def z_copy(src, blk, j):
        return remote(src, kv.at[blk * 2 + lo, j], z_s.at[blk, j], z_r.at[blk, j], dp,
                      jnp.minimum(me + 2, n - 1 - (1 - lo)))

    def x_copy(src, blk, j, side):
        return remote(src, kv.at[blk * 2 + side, j], x_s.at[blk, j], x_r.at[blk, j], dp, me + 1 - 2 * lo)

    @pl.loop(1, n)
    def _(d):
        seg_copy(me, other(d, me, n)).start()

    own = (k_ref, v_ref)

    for j in range(2):
        @pl.when(hi + 1 < n_hi)
        def _():
            z_copy(own[j], hi, j).start()

        @pl.when(lo == 0)
        def _():
            x_copy(own[j], hi, j, lo).start()

    @pl.loop(1, n)
    def _(d):
        prs_copy(me, other(d, me, n)).start()

    def queries(c):
        return jnp.concatenate([q_ref[:, head_cols(c * GROUP + g)] for g in range(GROUP)], axis=0)

    def grads(c):
        return jnp.concatenate([g_ref[:, head_cols(c * GROUP + g)] for g in range(GROUP)], axis=0)

    def wide(mask):
        return jnp.concatenate([mask] * GROUP, axis=1)

    q_seg = seg_ref[...]

    def column(row):
        return jnp.transpose(jnp.broadcast_to(row, (tok, tok)))

    def absorb(key_block, value_block, mask, first=False):
        mask = wide(mask)
        for c in range(KVH):
            st = dot_nt(key_block[:, head_cols(c)], queries(c)) * scale
            st = jnp.where(mask, st, -jnp.inf)
            peak = jnp.max(st, axis=0, keepdims=True)
            if not first:
                old = m_ref[c]
                peak = jnp.maximum(old, peak)
                shrink = jnp.exp(old - peak)
            w = jnp.exp(st - peak)
            total = jnp.sum(w, axis=0, keepdims=True)
            acc = dot_tn(value_block[:, head_cols(c)], w.astype(jnp.bfloat16))
            if not first:
                total = total + l_ref[c] * shrink
                acc = acc + acc_ref[c] * shrink
            m_ref[c] = peak
            l_ref[c] = total
            acc_ref[c] = acc

    order = lax.broadcasted_iota(jnp.int32, (tok, tok), 0) <= lax.broadcasted_iota(jnp.int32, (tok, tok), 1)
    absorb(k_ref, v_ref, (column(q_seg) == jnp.broadcast_to(q_seg, (tok, tok))) & order, True)

    def prs_add(d, total):
        src = other(d, me, n)
        prs_copy(src, me).wait_recv()
        return total + prs[src]

    pp[pl.ds(pl.multiple_of(me * rows, rows), rows), :] = lax.fori_loop(
        1, n, prs_add, sel[pl.ds(pl.multiple_of(me * rows, rows), rows), :])

    @pl.loop(1, n)
    def _(d):
        pag_copy(me, other(d, me, n)).start()

    @pl.loop(1, n)
    def _(d):
        seg_copy(other(d, me, n), me).wait_recv()

    def absorb_rank(rank):
        mask = column(segs[rank]) == jnp.broadcast_to(q_seg, (tok, tok))
        absorb(kv.at[rank, 0], kv.at[rank, 1], mask)

    @pl.when(lo == 1)
    def _():
        for j in range(2):
            x_copy(own[j], hi, j, 1 - lo).wait_recv()
        absorb_rank(me - 1)

    @pl.loop(1, hi + 1)
    def _(s):
        blk = hi - s
        for j in range(2):
            z_copy(own[j], blk, j).wait_recv()

            @pl.when(hi + 1 < n_hi)
            def _():
                z_copy(kv.at[blk * 2 + lo, j], blk, j).start()

            x_copy(kv.at[blk * 2 + lo, j], blk, j, lo).start()
        absorb_rank(blk * 2 + lo)
        for j in range(2):
            x_copy(own[j], blk, j, 1 - lo).wait_recv()
        absorb_rank(blk * 2 + 1 - lo)

    @pl.loop(1, n)
    def _(d):
        pag_copy(other(d, me, n), me).wait_recv()

    def grs_copy(src_rank, dst_rank):
        return remote(chunk(part, dst_rank), grs.at[src_rank], grs_s.at[dst_rank], grs_r.at[src_rank], dp, dst_rank)

    per_slot = n // SLOTS

    def send_slot(s):
        for i in range(per_slot):
            dst = s * per_slot + i

            @pl.when(me != dst)
            def _():
                grs_copy(me, dst).start()

    for c in range(KVH):
        q = queries(c)
        g = grads(c)
        pk = pp[c * PROMPT:(c + 1) * PROMPT, :]
        pv = pp[(KVH + c) * PROMPT:(KVH + c + 1) * PROMPT, :]
        r = dot_nt(pk, q) * scale
        old = m_ref[c]
        peak = jnp.maximum(old, jnp.max(r, axis=0, keepdims=True))
        shrink = jnp.exp(old - peak)
        w = jnp.exp(r - peak)
        total = jnp.sum(w, axis=0, keepdims=True) + l_ref[c] * shrink
        acc = dot_tn(pv, w.astype(jnp.bfloat16)) + acc_ref[c] * shrink
        att = jnp.transpose(acc / total).astype(jnp.bfloat16)
        for i in range(GROUP):
            att_ref[:, head_cols(c * GROUP + i)] = att[i * tok:(i + 1) * tok, :]
        delta = jnp.sum(jnp.transpose(g.astype(jnp.float32) * att.astype(jnp.float32)), axis=0, keepdims=True)
        probs = jnp.exp(r - (peak + jnp.log(total)))
        score_grad = probs * (dot_nt(pv, g) - delta)
        vp = dot_nn(probs.astype(jnp.bfloat16), g)
        kp = dot_nn(score_grad.astype(jnp.bfloat16), q) * scale
        part[c * PROMPT:(c + 1) * PROMPT, :] = kp.astype(jnp.bfloat16)
        part[(KVH + c) * PROMPT:(KVH + c + 1) * PROMPT, :] = vp.astype(jnp.bfloat16)
        send_slot(c)
        send_slot(KVH + c)

    def grs_add(d, total):
        src = other(d, me, n)
        grs_copy(src, me).wait_recv()
        return total + grs[src].astype(jnp.float32)

    mine = pl.ds(pl.multiple_of(me * rows, rows), rows)
    gath[dp, mine, :] = lax.fori_loop(1, n, grs_add, part[mine, :].astype(jnp.float32)).astype(jnp.bfloat16)

    def piece(b, j):
        return gath.at[b, pl.ds(pl.multiple_of(j * rows, rows), rows)]

    def gag_copy(src_rank, dst_rank):
        return remote(piece(dp, src_rank), piece(dp, src_rank), gag_s.at[dst_rank], gag_r.at[src_rank], dp, dst_rank)

    def y_copy(src_h, dst_h, j):
        b = src_h * 2 + dl
        return remote(piece(b, j), piece(b, j), y_s.at[dst_h, j], y_r.at[src_h, j], dst_h * 2 + dl, me)

    def c_copy(h, side, j):
        b = h * 2 + side
        return remote(piece(b, j), piece(b, j), c_s.at[h, j], c_r.at[h, j], dh * 2 + 1 - dl, me)

    @pl.loop(1, n)
    def _(d):
        gag_copy(me, other(d, me, n)).start()

    def pass_on(j):
        @pl.loop(1, n_dh)
        def _(e):
            y_copy(dh, other(e, dh, n_dh), j).start()
        c_copy(dh, dl, j).start()

    pass_on(me)

    @pl.loop(1, n)
    def _(d):
        src = other(d, me, n)
        gag_copy(src, me).wait_recv()
        pass_on(src)

    @pl.loop(0, n)
    def _(d):
        src = other(d, me, n)

        @pl.loop(1, n_dh)
        def _(e):
            h = other(e, dh, n_dh)
            y_copy(h, dh, src).wait_recv()
            c_copy(h, dl, src).start()

    @pl.loop(0, n)
    def _(d):
        src = other(d, me, n)

        @pl.loop(0, n_dh)
        def _(h):
            c_copy(h, 1 - dl, src).wait_recv()

    for s in range(SLOTS):
        dst = kg_ref if s < KVH else vg_ref
        for k in range(bank):
            total = jnp.zeros((PROMPT, HD), jnp.float32)
            for b in range(n_dp):
                hit = jnp.full((PROMPT, HD), task_ref[b], jnp.int32) == me * bank + k
                total = total + jnp.where(
                    hit, gath[b, s * PROMPT:(s + 1) * PROMPT, :].astype(jnp.float32), 0.0)
            dst[k, :, head_cols(s % KVH)] = total

    @pl.loop(1, n)
    def _(d):
        dst = other(d, me, n)
        seg_copy(me, dst).wait_send()
        prs_copy(me, dst).wait_send()
        pag_copy(me, dst).wait_send()
        grs_copy(me, dst).wait_send()
        gag_copy(me, dst).wait_send()

    for j in range(2):
        @pl.when(lo == 0)
        def _():
            x_copy(own[j], hi, j, lo).wait_send()

        @pl.loop(0, hi)
        def _(blk):
            x_copy(own[j], blk, j, lo).wait_send()

        @pl.when(hi + 1 < n_hi)
        def _():
            @pl.loop(0, hi + 1)
            def _(blk):
                z_copy(own[j], blk, j).wait_send()

    @pl.loop(0, n)
    def _(j):
        @pl.loop(1, n_dh)
        def _(e):
            y_copy(dh, other(e, dh, n_dh), j).wait_send()

        @pl.loop(0, n_dh)
        def _(h):
            c_copy(h, dl, j).wait_send()


def shards(n, n_dp, queries, keys, values, segments, task_ids, prompt_keys, prompt_values, grad_out):
    tok = queries.shape[1]
    width = KVH * HD
    rows = SLOTS * PROMPT // n
    bank = prompt_keys.shape[0]
    bf16, f32 = jnp.bfloat16, jnp.float32
    dma = pltpu.SemaphoreType.DMA
    vmem = pl.BlockSpec(memory_space=pltpu.VMEM)
    att, kg, vg = pl.pallas_call(
        functools.partial(kernel, n, n_dp),
        out_shape=(
            jax.ShapeDtypeStruct((tok, KVH * GROUP * HD), bf16),
            jax.ShapeDtypeStruct((bank, PROMPT, width), f32),
            jax.ShapeDtypeStruct((bank, PROMPT, width), f32),
        ),
        in_specs=[pl.BlockSpec(memory_space=pltpu.SMEM)] + [vmem] * 7,
        out_specs=(vmem, vmem, vmem),
        scratch_shapes=[
            pltpu.VMEM((n, 2, tok, width), bf16),
            pltpu.VMEM((n, 1, tok), jnp.int32),
            pltpu.VMEM((SLOTS * PROMPT, HD), bf16),
            pltpu.VMEM((n, rows, HD), bf16),
            pltpu.VMEM((SLOTS * PROMPT, HD), bf16),
            pltpu.VMEM((SLOTS * PROMPT, HD), bf16),
            pltpu.VMEM((n, rows, HD), bf16),
            pltpu.VMEM((n_dp, SLOTS * PROMPT, HD), bf16),
            pltpu.VMEM((KVH, 1, GROUP * tok), f32),
            pltpu.VMEM((KVH, 1, GROUP * tok), f32),
            pltpu.VMEM((KVH, HD, GROUP * tok), f32),
            dma((n,)), dma((n,)), dma((n,)), dma((n,)), dma((n,)), dma((n,)),
            dma((n // 2, 2)), dma((n // 2, 2)), dma((n // 2, 2)), dma((n // 2, 2)),
            dma((n,)), dma((n,)), dma((n,)), dma((n,)),
            dma((n_dp // 2, n)), dma((n_dp // 2, n)), dma((n_dp // 2, n)), dma((n_dp // 2, n)),
        ],
        compiler_params=pltpu.CompilerParams(collective_id=0, has_side_effects=True),
    )(task_ids, queries[0], keys[0], values[0], segments, prompt_keys, prompt_values, grad_out[0])
    return att[None], kg, vg


def solution(mesh):
    n, n_dp = mesh.shape["seq"], mesh.shape["dp"]
    in_specs = (
        P("dp", "seq", None),
        P("dp", "seq", None),
        P("dp", "seq", None),
        P("dp", "seq"),
        P(),
        P("seq", None, None),
        P("seq", None, None),
        P("dp", "seq", None),
    )
    out_specs = (P("dp", "seq", None), P("seq", None, None), P("seq", None, None))
    return jax.shard_map(
        functools.partial(shards, n, n_dp), mesh=mesh, in_specs=in_specs, out_specs=out_specs, check_vma=False
    )
```

```python
import functools
import math

import jax
import jax.numpy as jnp
from jax import lax
from jax.experimental import pallas as pl
from jax.experimental.pallas import tpu as pltpu
from jax.sharding import PartitionSpec as P

KVH = 4
GROUP = 4
HD = 128
PROMPT = 128
SLOTS = 2 * KVH


def dot_nt(a, b):
    return lax.dot_general(a, b, (((1,), (1,)), ((), ())), preferred_element_type=jnp.float32)


def dot_tn(a, b):
    return lax.dot_general(a, b, (((0,), (0,)), ((), ())), preferred_element_type=jnp.float32)


def dot_nn(a, b):
    return lax.dot_general(a, b, (((1,), (0,)), ((), ())), preferred_element_type=jnp.float32)


def head_cols(c):
    return slice(c * HD, (c + 1) * HD)


def kernel(
    n, n_dp, task_ref, *refs,
):
    inputs, refs = refs[:7], refs[7:]
    att_ref, kg_ref, vg_ref, held, load_s, *refs = refs
    (
    kv, segs, sel, prs, pp, part, grs, gath, m_ref, l_ref, acc_ref,
    seg_s, seg_r, prs_s, prs_r, pag_s, pag_r, z_s, z_r, x_s, x_r,
    grs_s, grs_r, gag_s, gag_r, y_s, y_r, c_s, c_r,
    ) = refs
    q_ref, k_ref, v_ref, seg_ref, pk_ref, pv_ref, g_ref = held
    loads = [pltpu.make_async_copy(src, dst, load_s.at[i]) for i, (src, dst) in enumerate(zip(inputs, held))]
    for i in (4, 5, 3, 1, 2, 0, 6):
        loads[i].start()
    tok = q_ref.shape[0]
    bank = pk_ref.shape[0]
    rows = SLOTS * PROMPT // n
    n_hi = n // 2
    n_dh = n_dp // 2
    scale = 1.0 / math.sqrt(HD)
    me = lax.axis_index("seq")
    dp = lax.axis_index("dp")
    hi, lo = me // 2, me % 2
    dh, dl = dp // 2, dp % 2

    def remote(src, dst, s_sem, r_sem, to_dp, to_seq):
        return pltpu.make_async_remote_copy(
            src_ref=src, dst_ref=dst, send_sem=s_sem, recv_sem=r_sem,
            device_id=(to_dp, to_seq), device_id_type=pl.DeviceIdType.MESH,
        )

    def other(d, base, count):
        return lax.rem(base + d, count)

    def chunk(ref, j):
        return ref.at[pl.ds(pl.multiple_of(j * rows, rows), rows)]

    barrier = pltpu.get_barrier_semaphore()

    @pl.loop(1, n)
    def _(d):
        pl.semaphore_signal(barrier, inc=1, device_id=(dp, other(d, me, n)),
                            device_id_type=pl.DeviceIdType.MESH)

    @pl.loop(1, n_dp)
    def _(d):
        pl.semaphore_signal(barrier, inc=1, device_id=(other(d, dp, n_dp), me),
                            device_id_type=pl.DeviceIdType.MESH)

    for i in (4, 5):
        loads[i].wait()

    task = task_ref[dp]
    for s in range(SLOTS):
        src = pk_ref if s < KVH else pv_ref
        total = jnp.zeros((PROMPT, HD), jnp.bfloat16)
        for k in range(bank):
            hit = jnp.full((PROMPT, HD), task, jnp.int32) == me * bank + k
            total = jnp.where(hit, src[k, :, head_cols(s % KVH)], total)
        sel[s * PROMPT:(s + 1) * PROMPT, :] = total

    for i in (3, 1, 2):
        loads[i].wait()
    pl.semaphore_wait(barrier, n - 1 + n_dp - 1)

    def seg_copy(src_rank, dst_rank):
        return remote(seg_ref, segs.at[src_rank], seg_s.at[dst_rank], seg_r.at[src_rank], dp, dst_rank)

    def prs_copy(src_rank, dst_rank):
        return remote(chunk(sel, dst_rank), prs.at[src_rank], prs_s.at[dst_rank], prs_r.at[src_rank], dp, dst_rank)

    def pag_copy(src_rank, dst_rank):
        return remote(chunk(pp, src_rank), chunk(pp, src_rank), pag_s.at[dst_rank], pag_r.at[src_rank], dp, dst_rank)

    def z_copy(src, blk, j):
        return remote(src, kv.at[blk * 2 + lo, j], z_s.at[blk, j], z_r.at[blk, j], dp,
                      jnp.minimum(me + 2, n - 1 - (1 - lo)))

    def x_copy(src, blk, j, side):
        return remote(src, kv.at[blk * 2 + side, j], x_s.at[blk, j], x_r.at[blk, j], dp, me + 1 - 2 * lo)

    @pl.loop(1, n)
    def _(d):
        seg_copy(me, other(d, me, n)).start()

    @pl.loop(1, n)
    def _(d):
        prs_copy(me, other(d, me, n)).start()

    own = (k_ref, v_ref)

    for j in range(2):
        @pl.when(hi + 1 < n_hi)
        def _():
            z_copy(own[j], hi, j).start()

        @pl.when(lo == 0)
        def _():
            x_copy(own[j], hi, j, lo).start()

    def queries(c):
        return jnp.concatenate([q_ref[:, head_cols(c * GROUP + g)] for g in range(GROUP)], axis=0)

    def grads(c):
        return jnp.concatenate([g_ref[:, head_cols(c * GROUP + g)] for g in range(GROUP)], axis=0)

    def wide(mask):
        return jnp.concatenate([mask] * GROUP, axis=1)

    loads[0].wait()
    q_seg = seg_ref[...]

    def column(row):
        return jnp.transpose(jnp.broadcast_to(row, (tok, tok)))

    def absorb(key_block, value_block, mask, first=False):
        mask = wide(mask)
        for c in range(KVH):
            st = dot_nt(key_block[:, head_cols(c)], queries(c)) * scale
            st = jnp.where(mask, st, -jnp.inf)
            peak = jnp.max(st, axis=0, keepdims=True)
            if not first:
                old = m_ref[c]
                peak = jnp.maximum(old, peak)
                shrink = jnp.exp(old - peak)
            w = jnp.exp(st - peak)
            total = jnp.sum(w, axis=0, keepdims=True)
            acc = dot_tn(value_block[:, head_cols(c)], w.astype(jnp.bfloat16))
            if not first:
                total = total + l_ref[c] * shrink
                acc = acc + acc_ref[c] * shrink
            m_ref[c] = peak
            l_ref[c] = total
            acc_ref[c] = acc

    order = lax.broadcasted_iota(jnp.int32, (tok, tok), 0) <= lax.broadcasted_iota(jnp.int32, (tok, tok), 1)
    absorb(k_ref, v_ref, (column(q_seg) == jnp.broadcast_to(q_seg, (tok, tok))) & order, True)

    def spread_prompt():
        def prs_add(d, total):
            src = other(d, me, n)
            prs_copy(src, me).wait_recv()
            return total + prs[src]

        mine = pl.ds(pl.multiple_of(me * rows, rows), rows)
        pp[mine, :] = lax.fori_loop(1, n, prs_add, sel[mine, :])

        @pl.loop(1, n)
        def _(d):
            pag_copy(me, other(d, me, n)).start()

    pl.when(hi == 0)(spread_prompt)

    @pl.loop(1, n)
    def _(d):
        seg_copy(other(d, me, n), me).wait_recv()

    def absorb_rank(rank):
        mask = column(segs[rank]) == jnp.broadcast_to(q_seg, (tok, tok))
        absorb(kv.at[rank, 0], kv.at[rank, 1], mask)

    def absorb_crossed(blk):
        for j in range(2):
            x_copy(own[j], blk, j, 1 - lo).wait_recv()
        absorb_rank(blk * 2 + 1 - lo)

    @pl.loop(1, hi + 1)
    def _(s):
        blk = hi - s
        for j in range(2):
            z_copy(own[j], blk, j).wait_recv()

            @pl.when(hi + 1 < n_hi)
            def _():
                z_copy(kv.at[blk * 2 + lo, j], blk, j).start()

            x_copy(kv.at[blk * 2 + lo, j], blk, j, lo).start()
        pl.when(s == 1)(spread_prompt)
        absorb_rank(blk * 2 + lo)

        @pl.when(jnp.logical_or(s > 1, lo == 1))
        def _():
            absorb_crossed(blk + 1)

    @pl.when(jnp.logical_or(hi > 0, lo == 1))
    def _():
        absorb_crossed(0)

    @pl.loop(1, n)
    def _(d):
        pag_copy(other(d, me, n), me).wait_recv()

    loads[6].wait()

    def grs_copy(src_rank, dst_rank):
        return remote(chunk(part, dst_rank), grs.at[src_rank], grs_s.at[dst_rank], grs_r.at[src_rank], dp, dst_rank)

    per_slot = n // SLOTS

    def send_slot(s):
        for i in range(per_slot):
            dst = s * per_slot + i

            @pl.when(me != dst)
            def _():
                grs_copy(me, dst).start()

    for c in range(KVH):
        q = queries(c)
        g = grads(c)
        pk = pp[c * PROMPT:(c + 1) * PROMPT, :]
        pv = pp[(KVH + c) * PROMPT:(KVH + c + 1) * PROMPT, :]
        r = dot_nt(pk, q) * scale
        old = m_ref[c]
        peak = jnp.maximum(old, jnp.max(r, axis=0, keepdims=True))
        shrink = jnp.exp(old - peak)
        w = jnp.exp(r - peak)
        total = jnp.sum(w, axis=0, keepdims=True) + l_ref[c] * shrink
        acc = dot_tn(pv, w.astype(jnp.bfloat16)) + acc_ref[c] * shrink
        att = jnp.transpose(acc / total).astype(jnp.bfloat16)
        for i in range(GROUP):
            att_ref[:, head_cols(c * GROUP + i)] = att[i * tok:(i + 1) * tok, :]
        delta = jnp.sum(jnp.transpose(g.astype(jnp.float32) * att.astype(jnp.float32)), axis=0, keepdims=True)
        probs = jnp.exp(r - (peak + jnp.log(total)))
        score_grad = probs * (dot_nt(pv, g) - delta)
        vp = dot_nn(probs.astype(jnp.bfloat16), g)
        kp = dot_nn(score_grad.astype(jnp.bfloat16), q) * scale
        part[c * PROMPT:(c + 1) * PROMPT, :] = kp.astype(jnp.bfloat16)
        part[(KVH + c) * PROMPT:(KVH + c + 1) * PROMPT, :] = vp.astype(jnp.bfloat16)
        send_slot(c)
        send_slot(KVH + c)

    def grs_add(d, total):
        src = other(d, me, n)
        grs_copy(src, me).wait_recv()
        return total + grs[src].astype(jnp.float32)

    mine = pl.ds(pl.multiple_of(me * rows, rows), rows)
    gath[dp, mine, :] = lax.fori_loop(1, n, grs_add, part[mine, :].astype(jnp.float32)).astype(jnp.bfloat16)

    def piece(b, j):
        return gath.at[b, pl.ds(pl.multiple_of(j * rows, rows), rows)]

    def gag_copy(src_rank, dst_rank):
        return remote(piece(dp, src_rank), piece(dp, src_rank), gag_s.at[dst_rank], gag_r.at[src_rank], dp, dst_rank)

    def y_copy(src_h, dst_h, j):
        b = src_h * 2 + dl
        return remote(piece(b, j), piece(b, j), y_s.at[dst_h, j], y_r.at[src_h, j], dst_h * 2 + dl, me)

    def c_copy(h, side, j):
        b = h * 2 + side
        return remote(piece(b, j), piece(b, j), c_s.at[h, j], c_r.at[h, j], dh * 2 + 1 - dl, me)

    @pl.loop(1, n)
    def _(d):
        gag_copy(me, other(d, me, n)).start()

    def pass_on(j):
        @pl.loop(1, n_dh)
        def _(e):
            y_copy(dh, other(e, dh, n_dh), j).start()
        c_copy(dh, dl, j).start()

    pass_on(me)

    @pl.loop(1, n)
    def _(d):
        src = other(d, me, n)
        gag_copy(src, me).wait_recv()
        pass_on(src)

    @pl.loop(0, n)
    def _(d):
        src = other(d, me, n)

        @pl.loop(1, n_dh)
        def _(e):
            h = other(e, dh, n_dh)
            y_copy(h, dh, src).wait_recv()
            c_copy(h, dl, src).start()

    @pl.loop(0, n)
    def _(d):
        src = other(d, me, n)

        @pl.loop(0, n_dh)
        def _(h):
            c_copy(h, 1 - dl, src).wait_recv()

    for s in range(SLOTS):
        dst = kg_ref if s < KVH else vg_ref
        for k in range(bank):
            total = jnp.zeros((PROMPT, HD), jnp.float32)
            for b in range(n_dp):
                hit = jnp.full((PROMPT, HD), task_ref[b], jnp.int32) == me * bank + k
                total = total + jnp.where(
                    hit, gath[b, s * PROMPT:(s + 1) * PROMPT, :].astype(jnp.float32), 0.0)
            dst[k, :, head_cols(s % KVH)] = total

    @pl.loop(1, n)
    def _(d):
        dst = other(d, me, n)
        seg_copy(me, dst).wait_send()
        prs_copy(me, dst).wait_send()
        pag_copy(me, dst).wait_send()
        grs_copy(me, dst).wait_send()
        gag_copy(me, dst).wait_send()

    for j in range(2):
        @pl.when(lo == 0)
        def _():
            x_copy(own[j], hi, j, lo).wait_send()

        @pl.loop(0, hi)
        def _(blk):
            x_copy(own[j], blk, j, lo).wait_send()

        @pl.when(hi + 1 < n_hi)
        def _():
            @pl.loop(0, hi + 1)
            def _(blk):
                z_copy(own[j], blk, j).wait_send()

    @pl.loop(0, n)
    def _(j):
        @pl.loop(1, n_dh)
        def _(e):
            y_copy(dh, other(e, dh, n_dh), j).wait_send()

        @pl.loop(0, n_dh)
        def _(h):
            c_copy(h, dl, j).wait_send()


def shards(n, n_dp, queries, keys, values, segments, task_ids, prompt_keys, prompt_values, grad_out):
    tok = queries.shape[1]
    width = KVH * HD
    rows = SLOTS * PROMPT // n
    bank = prompt_keys.shape[0]
    bf16, f32 = jnp.bfloat16, jnp.float32
    dma = pltpu.SemaphoreType.DMA
    vmem = pl.BlockSpec(memory_space=pltpu.VMEM)
    operands = (queries[0], keys[0], values[0], segments, prompt_keys, prompt_values, grad_out[0])
    att, kg, vg = pl.pallas_call(
        functools.partial(kernel, n, n_dp),
        out_shape=(
            jax.ShapeDtypeStruct((tok, KVH * GROUP * HD), bf16),
            jax.ShapeDtypeStruct((bank, PROMPT, width), f32),
            jax.ShapeDtypeStruct((bank, PROMPT, width), f32),
        ),
        in_specs=[pl.BlockSpec(memory_space=pltpu.SMEM)] + [pl.BlockSpec(memory_space=pl.ANY)] * 7,
        out_specs=(vmem, vmem, vmem),
        scratch_shapes=[
            [pltpu.VMEM(a.shape, a.dtype) for a in operands],
            dma((7,)),
            pltpu.VMEM((n, 2, tok, width), bf16),
            pltpu.VMEM((n, 1, tok), jnp.int32),
            pltpu.VMEM((SLOTS * PROMPT, HD), bf16),
            pltpu.VMEM((n, rows, HD), bf16),
            pltpu.VMEM((SLOTS * PROMPT, HD), bf16),
            pltpu.VMEM((SLOTS * PROMPT, HD), bf16),
            pltpu.VMEM((n, rows, HD), bf16),
            pltpu.VMEM((n_dp, SLOTS * PROMPT, HD), bf16),
            pltpu.VMEM((KVH, 1, GROUP * tok), f32),
            pltpu.VMEM((KVH, 1, GROUP * tok), f32),
            pltpu.VMEM((KVH, HD, GROUP * tok), f32),
            dma((n,)), dma((n,)), dma((n,)), dma((n,)), dma((n,)), dma((n,)),
            dma((n // 2, 2)), dma((n // 2, 2)), dma((n // 2, 2)), dma((n // 2, 2)),
            dma((n,)), dma((n,)), dma((n,)), dma((n,)),
            dma((n_dp // 2, n)), dma((n_dp // 2, n)), dma((n_dp // 2, n)), dma((n_dp // 2, n)),
        ],
        compiler_params=pltpu.CompilerParams(collective_id=0, has_side_effects=True),
    )(task_ids, *operands)
    return att[None], kg, vg


def solution(mesh):
    n, n_dp = mesh.shape["seq"], mesh.shape["dp"]
    in_specs = (
        P("dp", "seq", None),
        P("dp", "seq", None),
        P("dp", "seq", None),
        P("dp", "seq"),
        P(),
        P("seq", None, None),
        P("seq", None, None),
        P("dp", "seq", None),
    )
    out_specs = (P("dp", "seq", None), P("seq", None, None), P("seq", None, None))
    return jax.shard_map(
        functools.partial(shards, n, n_dp), mesh=mesh, in_specs=in_specs, out_specs=out_specs, check_vma=False
    )
```

```python
import functools
import math

import jax
import jax.numpy as jnp
from jax import lax
from jax.experimental import pallas as pl
from jax.experimental.pallas import tpu as pltpu
from jax.sharding import PartitionSpec as P

KVH = 4
GROUP = 4
HD = 128
PROMPT = 128
SLOTS = 2 * KVH


def dot_nt(a, b):
    return lax.dot_general(a, b, (((1,), (1,)), ((), ())), preferred_element_type=jnp.float32)


def dot_tn(a, b):
    return lax.dot_general(a, b, (((0,), (0,)), ((), ())), preferred_element_type=jnp.float32)


def dot_nn(a, b):
    return lax.dot_general(a, b, (((1,), (0,)), ((), ())), preferred_element_type=jnp.float32)


def head_cols(c):
    return slice(c * HD, (c + 1) * HD)


def kernel(
    n, n_dp, task_ref, *refs,
):
    inputs, refs = refs[:7], refs[7:]
    att_out, gath, held, load_s, att_ref, att_s, *refs = refs
    (
    kv, segs, sel, prs, pp, part, grs, m_ref, l_ref, acc_ref, r_ref, d_ref,
    seg_s, seg_r, prs_s, prs_r, pag_s, pag_r, z_s, z_r, x_s, x_r,
    grs_s, grs_r, gag_s, gag_r, y_s, y_r, c_s, c_r,
    ) = refs
    q_ref, k_ref, v_ref, seg_ref, pk_ref, pv_ref, g_ref = held
    loads = [pltpu.make_async_copy(src, dst, load_s.at[i]) for i, (src, dst) in enumerate(zip(inputs, held))]
    for i in (4, 5, 3, 1, 2, 0, 6):
        loads[i].start()
    tok = q_ref.shape[0]
    bank = pk_ref.shape[0]
    rows = SLOTS * PROMPT // n
    n_hi = n // 2
    n_dh = n_dp // 2
    scale = 1.0 / math.sqrt(HD)
    me = lax.axis_index("seq")
    dp = lax.axis_index("dp")
    hi, lo = me // 2, me % 2
    dh, dl = dp // 2, dp % 2

    def remote(src, dst, s_sem, r_sem, to_dp, to_seq):
        return pltpu.make_async_remote_copy(
            src_ref=src, dst_ref=dst, send_sem=s_sem, recv_sem=r_sem,
            device_id=(to_dp, to_seq), device_id_type=pl.DeviceIdType.MESH,
        )

    def other(d, base, count):
        return lax.rem(base + d, count)

    def chunk(ref, j):
        return ref.at[pl.ds(pl.multiple_of(j * rows, rows), rows)]

    barrier = pltpu.get_barrier_semaphore()

    @pl.loop(1, n)
    def _(d):
        pl.semaphore_signal(barrier, inc=1, device_id=(dp, other(d, me, n)),
                            device_id_type=pl.DeviceIdType.MESH)

    @pl.loop(1, n_dp)
    def _(d):
        pl.semaphore_signal(barrier, inc=1, device_id=(other(d, dp, n_dp), me),
                            device_id_type=pl.DeviceIdType.MESH)

    for i in (4, 5):
        loads[i].wait()

    task = task_ref[dp]
    for s in range(SLOTS):
        src = pk_ref if s < KVH else pv_ref
        total = jnp.zeros((PROMPT, HD), jnp.bfloat16)
        for k in range(bank):
            hit = jnp.full((PROMPT, HD), task, jnp.int32) == me * bank + k
            total = jnp.where(hit, src[k, :, head_cols(s % KVH)], total)
        sel[s * PROMPT:(s + 1) * PROMPT, :] = total

    for i in (3, 1, 2):
        loads[i].wait()
    pl.semaphore_wait(barrier, n - 1 + n_dp - 1)

    def seg_copy(src_rank, dst_rank):
        return remote(seg_ref, segs.at[src_rank], seg_s.at[dst_rank], seg_r.at[src_rank], dp, dst_rank)

    def prs_copy(src_rank, dst_rank):
        return remote(chunk(sel, dst_rank), prs.at[src_rank], prs_s.at[dst_rank], prs_r.at[src_rank], dp, dst_rank)

    def pag_copy(src_rank, dst_rank):
        return remote(chunk(pp, src_rank), chunk(pp, src_rank), pag_s.at[dst_rank], pag_r.at[src_rank], dp, dst_rank)

    def z_copy(src, blk, j):
        return remote(src, kv.at[blk * 2 + lo, j], z_s.at[blk, j], z_r.at[blk, j], dp,
                      jnp.minimum(me + 2, n - 1 - (1 - lo)))

    def x_copy(src, blk, j, side):
        return remote(src, kv.at[blk * 2 + side, j], x_s.at[blk, j], x_r.at[blk, j], dp, me + 1 - 2 * lo)

    @pl.loop(1, n)
    def _(d):
        seg_copy(me, other(d, me, n)).start()

    own = (k_ref, v_ref)

    for j in range(2):
        @pl.when(hi + 1 < n_hi)
        def _():
            z_copy(own[j], hi, j).start()

        @pl.when(lo == 0)
        def _():
            x_copy(own[j], hi, j, lo).start()

    @pl.loop(1, n)
    def _(d):
        prs_copy(me, other(d, me, n)).start()

    def queries(c):
        return jnp.concatenate([q_ref[:, head_cols(c * GROUP + g)] for g in range(GROUP)], axis=0)

    def grads(c):
        return jnp.concatenate([g_ref[:, head_cols(c * GROUP + g)] for g in range(GROUP)], axis=0)

    def wide(mask):
        return jnp.concatenate([mask] * GROUP, axis=1)

    loads[0].wait()
    q_seg = seg_ref[...]

    def column(row):
        return jnp.transpose(jnp.broadcast_to(row, (tok, tok)))

    def absorb(key_block, value_block, mask, first=False):
        mask = wide(mask)
        for c in range(KVH):
            st = dot_nt(key_block[:, head_cols(c)], queries(c)) * scale
            st = jnp.where(mask, st, -jnp.inf)
            peak = jnp.max(st, axis=0, keepdims=True)
            if not first:
                old = m_ref[c]
                peak = jnp.maximum(old, peak)
                shrink = jnp.exp(old - peak)
            w = jnp.exp(st - peak)
            total = jnp.sum(w, axis=0, keepdims=True)
            acc = dot_tn(value_block[:, head_cols(c)], w.astype(jnp.bfloat16))
            if not first:
                total = total + l_ref[c] * shrink
                acc = acc + acc_ref[c] * shrink
            m_ref[c] = peak
            l_ref[c] = total
            acc_ref[c] = acc

    order = lax.broadcasted_iota(jnp.int32, (tok, tok), 0) <= lax.broadcasted_iota(jnp.int32, (tok, tok), 1)
    absorb(k_ref, v_ref, (column(q_seg) == jnp.broadcast_to(q_seg, (tok, tok))) & order, True)

    def spread_prompt():
        def prs_add(d, total):
            src = other(d, me, n)
            prs_copy(src, me).wait_recv()
            return total + prs[src]

        mine = pl.ds(pl.multiple_of(me * rows, rows), rows)
        pp[mine, :] = lax.fori_loop(1, n, prs_add, sel[mine, :])

        @pl.loop(1, n)
        def _(d):
            pag_copy(me, other(d, me, n)).start()

    pl.when(hi == 0)(spread_prompt)

    @pl.loop(1, n)
    def _(d):
        seg_copy(other(d, me, n), me).wait_recv()

    def absorb_rank(rank):
        mask = column(segs[rank]) == jnp.broadcast_to(q_seg, (tok, tok))
        absorb(kv.at[rank, 0], kv.at[rank, 1], mask)

    def absorb_crossed(blk):
        for j in range(2):
            x_copy(own[j], blk, j, 1 - lo).wait_recv()
        absorb_rank(blk * 2 + 1 - lo)

    @pl.loop(1, hi + 1)
    def _(s):
        blk = hi - s
        for j in range(2):
            z_copy(own[j], blk, j).wait_recv()

            @pl.when(hi + 1 < n_hi)
            def _():
                z_copy(kv.at[blk * 2 + lo, j], blk, j).start()

            x_copy(kv.at[blk * 2 + lo, j], blk, j, lo).start()
        pl.when(s == jnp.minimum(hi, 2))(spread_prompt)
        absorb_rank(blk * 2 + lo)

        @pl.when(jnp.logical_or(s > 1, lo == 1))
        def _():
            absorb_crossed(blk + 1)

    @pl.loop(1, n)
    def _(d):
        pag_copy(other(d, me, n), me).wait_recv()

    loads[6].wait()
    for c in range(KVH):
        pk = pp[c * PROMPT:(c + 1) * PROMPT, :]
        pv = pp[(KVH + c) * PROMPT:(KVH + c + 1) * PROMPT, :]
        r = dot_nt(pk, queries(c)) * scale
        old = m_ref[c]
        peak = jnp.maximum(old, jnp.max(r, axis=0, keepdims=True))
        shrink = jnp.exp(old - peak)
        w = jnp.exp(r - peak)
        m_ref[c] = peak
        l_ref[c] = jnp.sum(w, axis=0, keepdims=True) + l_ref[c] * shrink
        acc_ref[c] = dot_tn(pv, w.astype(jnp.bfloat16)) + acc_ref[c] * shrink
        r_ref[c] = r
        d_ref[c] = dot_nt(pv, grads(c))

    @pl.when(jnp.logical_or(hi > 0, lo == 1))
    def _():
        absorb_crossed(0)

    def grs_copy(src_rank, dst_rank):
        return remote(chunk(part, dst_rank), grs.at[src_rank], grs_s.at[dst_rank], grs_r.at[src_rank], dp, dst_rank)

    per_slot = n // SLOTS

    def send_slot(s):
        for i in range(per_slot):
            dst = s * per_slot + i

            @pl.when(me != dst)
            def _():
                grs_copy(me, dst).start()

    for c in range(KVH):
        q = queries(c)
        g = grads(c)
        total = l_ref[c]
        att = jnp.transpose(acc_ref[c] / total).astype(jnp.bfloat16)
        for i in range(GROUP):
            att_ref[:, head_cols(c * GROUP + i)] = att[i * tok:(i + 1) * tok, :]
        delta = jnp.sum(jnp.transpose(g.astype(jnp.float32) * att.astype(jnp.float32)), axis=0, keepdims=True)
        probs = jnp.exp(r_ref[c] - (m_ref[c] + jnp.log(total)))
        score_grad = probs * (d_ref[c] - delta)
        vp = dot_nn(probs.astype(jnp.bfloat16), g)
        kp = dot_nn(score_grad.astype(jnp.bfloat16), q) * scale
        part[c * PROMPT:(c + 1) * PROMPT, :] = kp.astype(jnp.bfloat16)
        part[(KVH + c) * PROMPT:(KVH + c + 1) * PROMPT, :] = vp.astype(jnp.bfloat16)
        send_slot(c)
        send_slot(KVH + c)

    att_copy = pltpu.make_async_copy(att_ref, att_out, att_s)
    att_copy.start()

    def grs_add(d, total):
        src = other(d, me, n)
        grs_copy(src, me).wait_recv()
        return total + grs[src].astype(jnp.float32)

    mine = pl.ds(pl.multiple_of(me * rows, rows), rows)
    gath[dp, mine, :] = lax.fori_loop(1, n, grs_add, part[mine, :].astype(jnp.float32)).astype(jnp.bfloat16)

    def piece(b, j):
        return gath.at[b, pl.ds(pl.multiple_of(j * rows, rows), rows)]

    def gag_copy(src_rank, dst_rank):
        return remote(piece(dp, src_rank), piece(dp, src_rank), gag_s.at[dst_rank], gag_r.at[src_rank], dp, dst_rank)

    def y_copy(src_h, dst_h, j):
        b = src_h * 2 + dl
        return remote(piece(b, j), piece(b, j), y_s.at[dst_h, j], y_r.at[src_h, j], dst_h * 2 + dl, me)

    def c_copy(h, side, j):
        b = h * 2 + side
        return remote(piece(b, j), piece(b, j), c_s.at[h, j], c_r.at[h, j], dh * 2 + 1 - dl, me)

    @pl.loop(1, n)
    def _(d):
        gag_copy(me, other(d, me, n)).start()

    def pass_on(j):
        @pl.loop(1, n_dh)
        def _(e):
            y_copy(dh, other(e, dh, n_dh), j).start()
        c_copy(dh, dl, j).start()

    pass_on(me)

    @pl.loop(1, n)
    def _(d):
        src = other(d, me, n)
        gag_copy(src, me).wait_recv()
        pass_on(src)

    @pl.loop(0, n)
    def _(d):
        src = other(d, me, n)

        @pl.loop(1, n_dh)
        def _(e):
            h = other(e, dh, n_dh)
            y_copy(h, dh, src).wait_recv()
            c_copy(h, dl, src).start()

    @pl.loop(0, n)
    def _(d):
        src = other(d, me, n)

        @pl.loop(0, n_dh)
        def _(h):
            c_copy(h, 1 - dl, src).wait_recv()

    att_copy.wait()

    @pl.loop(1, n)
    def _(d):
        dst = other(d, me, n)
        seg_copy(me, dst).wait_send()
        prs_copy(me, dst).wait_send()
        pag_copy(me, dst).wait_send()
        grs_copy(me, dst).wait_send()
        gag_copy(me, dst).wait_send()

    for j in range(2):
        @pl.when(lo == 0)
        def _():
            x_copy(own[j], hi, j, lo).wait_send()

        @pl.loop(0, hi)
        def _(blk):
            x_copy(own[j], blk, j, lo).wait_send()

        @pl.when(hi + 1 < n_hi)
        def _():
            @pl.loop(0, hi + 1)
            def _(blk):
                z_copy(own[j], blk, j).wait_send()

    @pl.loop(0, n)
    def _(j):
        @pl.loop(1, n_dh)
        def _(e):
            y_copy(dh, other(e, dh, n_dh), j).wait_send()

        @pl.loop(0, n_dh)
        def _(h):
            c_copy(h, dl, j).wait_send()


def finish(n_dp, task_ref, att_in, gath_in, att_out, kg_out, vg_out, att_v, gath_v, kg_v, vg_v, sems, out_s):
    bank = kg_v.shape[0]
    me = lax.axis_index("seq")
    att_load = pltpu.make_async_copy(att_in, att_v, sems.at[SLOTS])
    att_store = pltpu.make_async_copy(att_v, att_out, out_s.at[2 * bank])

    def load(s):
        rows = pl.ds(s * PROMPT, PROMPT)
        return pltpu.make_async_copy(gath_in.at[:, rows], gath_v.at[:, rows], sems.at[s])

    for s in range(SLOTS):
        load(s).start()
        if s == 1:
            att_load.start()
    stores = [att_store]
    for s in range(SLOTS):
        load(s).wait()
        held, out = (kg_v, kg_out) if s < KVH else (vg_v, vg_out)
        for k in range(bank):
            total = jnp.zeros((PROMPT, HD), jnp.float32)
            for b in range(n_dp):
                hit = jnp.full((PROMPT, HD), task_ref[b], jnp.int32) == me * bank + k
                total = total + jnp.where(
                    hit, gath_v[b, s * PROMPT:(s + 1) * PROMPT, :].astype(jnp.float32), 0.0)
            held[k, :, head_cols(s % KVH)] = total
            if s % KVH == KVH - 1:
                stores.append(pltpu.make_async_copy(held.at[k], out.at[k], out_s.at[s // KVH * bank + k]))
                stores[-1].start()
        if s == 2:
            att_load.wait()
            att_store.start()
    for store in stores:
        store.wait()


def shards(n, n_dp, queries, keys, values, segments, task_ids, prompt_keys, prompt_values, grad_out):
    tok = queries.shape[1]
    width = KVH * HD
    rows = SLOTS * PROMPT // n
    bank = prompt_keys.shape[0]
    bf16, f32 = jnp.bfloat16, jnp.float32
    dma = pltpu.SemaphoreType.DMA
    vmem = pl.BlockSpec(memory_space=pltpu.VMEM)
    operands = (queries[0], keys[0], values[0], segments, prompt_keys, prompt_values, grad_out[0])
    att, gath = pl.pallas_call(
        functools.partial(kernel, n, n_dp),
        out_shape=(
            jax.ShapeDtypeStruct((tok, KVH * GROUP * HD), bf16),
            jax.ShapeDtypeStruct((n_dp, SLOTS * PROMPT, HD), bf16),
        ),
        in_specs=[pl.BlockSpec(memory_space=pltpu.SMEM)] + [pl.BlockSpec(memory_space=pl.ANY)] * 7,
        out_specs=(pl.BlockSpec(memory_space=pl.ANY), vmem),
        scratch_shapes=[
            [pltpu.VMEM(a.shape, a.dtype) for a in operands],
            dma((7,)),
            pltpu.VMEM((tok, KVH * GROUP * HD), bf16),
            dma,
            pltpu.VMEM((n, 2, tok, width), bf16),
            pltpu.VMEM((n, 1, tok), jnp.int32),
            pltpu.VMEM((SLOTS * PROMPT, HD), bf16),
            pltpu.VMEM((n, rows, HD), bf16),
            pltpu.VMEM((SLOTS * PROMPT, HD), bf16),
            pltpu.VMEM((SLOTS * PROMPT, HD), bf16),
            pltpu.VMEM((n, rows, HD), bf16),
            pltpu.VMEM((KVH, 1, GROUP * tok), f32),
            pltpu.VMEM((KVH, 1, GROUP * tok), f32),
            pltpu.VMEM((KVH, HD, GROUP * tok), f32),
            pltpu.VMEM((KVH, PROMPT, GROUP * tok), f32),
            pltpu.VMEM((KVH, PROMPT, GROUP * tok), f32),
            dma((n,)), dma((n,)), dma((n,)), dma((n,)), dma((n,)), dma((n,)),
            dma((n // 2, 2)), dma((n // 2, 2)), dma((n // 2, 2)), dma((n // 2, 2)),
            dma((n,)), dma((n,)), dma((n,)), dma((n,)),
            dma((n_dp // 2, n)), dma((n_dp // 2, n)), dma((n_dp // 2, n)), dma((n_dp // 2, n)),
        ],
        compiler_params=pltpu.CompilerParams(collective_id=0, has_side_effects=True),
    )(task_ids, *operands)
    anyspace = pl.BlockSpec(memory_space=pl.ANY)
    att, kg, vg = pl.pallas_call(
        functools.partial(finish, n_dp),
        out_shape=(
            jax.ShapeDtypeStruct((tok, KVH * GROUP * HD), bf16),
            jax.ShapeDtypeStruct((bank, PROMPT, width), f32),
            jax.ShapeDtypeStruct((bank, PROMPT, width), f32),
        ),
        in_specs=[pl.BlockSpec(memory_space=pltpu.SMEM), anyspace, anyspace],
        out_specs=(anyspace, anyspace, anyspace),
        scratch_shapes=[
            pltpu.VMEM((tok, KVH * GROUP * HD), bf16),
            pltpu.VMEM((n_dp, SLOTS * PROMPT, HD), bf16),
            pltpu.VMEM((bank, PROMPT, width), f32),
            pltpu.VMEM((bank, PROMPT, width), f32),
            dma((SLOTS + 1,)),
            dma((2 * bank + 1,)),
        ],
    )(task_ids, att, gath)
    return att[None], kg, vg


def solution(mesh):
    n, n_dp = mesh.shape["seq"], mesh.shape["dp"]
    in_specs = (
        P("dp", "seq", None),
        P("dp", "seq", None),
        P("dp", "seq", None),
        P("dp", "seq"),
        P(),
        P("seq", None, None),
        P("seq", None, None),
        P("dp", "seq", None),
    )
    out_specs = (P("dp", "seq", None), P("seq", None, None), P("seq", None, None))
    return jax.shard_map(
        functools.partial(shards, n, n_dp), mesh=mesh, in_specs=in_specs, out_specs=out_specs, check_vma=False
    )
```

```python
import functools
import math

import jax
import jax.numpy as jnp
from jax import lax
from jax.experimental import pallas as pl
from jax.experimental.pallas import tpu as pltpu
from jax.sharding import PartitionSpec as P

KVH = 4
GROUP = 4
HD = 128
PROMPT = 128
SLOTS = 2 * KVH


def dot_nt(a, b):
    return lax.dot_general(a, b, (((1,), (1,)), ((), ())), preferred_element_type=jnp.float32)


def dot_tn(a, b):
    return lax.dot_general(a, b, (((0,), (0,)), ((), ())), preferred_element_type=jnp.float32)


def dot_nn(a, b):
    return lax.dot_general(a, b, (((1,), (0,)), ((), ())), preferred_element_type=jnp.float32)


def head_cols(c):
    return slice(c * HD, (c + 1) * HD)


def kernel(
    n, n_dp, task_ref, *refs,
):
    inputs, refs = refs[:7], refs[7:]
    att_ref, gath, held, load_s, *refs = refs
    (
    kv, segs, sel, prs, pp, part, grs, m_ref, l_ref, acc_ref, r_ref, d_ref,
    seg_s, seg_r, prs_s, prs_r, pag_s, pag_r, z_s, z_r, x_s, x_r,
    grs_s, grs_r, gag_s, gag_r, y_s, y_r, c_s, c_r,
    ) = refs
    q_ref, k_ref, v_ref, seg_ref, pk_ref, pv_ref, g_ref = held
    loads = [pltpu.make_async_copy(src, dst, load_s.at[i]) for i, (src, dst) in enumerate(zip(inputs, held))]
    for i in (4, 5, 3, 1, 2, 0, 6):
        loads[i].start()
    tok = q_ref.shape[0]
    bank = pk_ref.shape[0]
    rows = SLOTS * PROMPT // n
    n_hi = n // 2
    n_dh = n_dp // 2
    scale = 1.0 / math.sqrt(HD)
    me = lax.axis_index("seq")
    dp = lax.axis_index("dp")
    hi, lo = me // 2, me % 2
    dh, dl = dp // 2, dp % 2

    def remote(src, dst, s_sem, r_sem, to_dp, to_seq):
        return pltpu.make_async_remote_copy(
            src_ref=src, dst_ref=dst, send_sem=s_sem, recv_sem=r_sem,
            device_id=(to_dp, to_seq), device_id_type=pl.DeviceIdType.MESH,
        )

    def other(d, base, count):
        return lax.rem(base + d, count)

    def chunk(ref, j):
        return ref.at[pl.ds(pl.multiple_of(j * rows, rows), rows)]

    barrier = pltpu.get_barrier_semaphore()

    @pl.loop(1, n)
    def _(d):
        pl.semaphore_signal(barrier, inc=1, device_id=(dp, other(d, me, n)),
                            device_id_type=pl.DeviceIdType.MESH)

    @pl.loop(1, n_dp)
    def _(d):
        pl.semaphore_signal(barrier, inc=1, device_id=(other(d, dp, n_dp), me),
                            device_id_type=pl.DeviceIdType.MESH)

    for i in (4, 5):
        loads[i].wait()

    task = task_ref[dp]
    for s in range(SLOTS):
        src = pk_ref if s < KVH else pv_ref
        total = jnp.zeros((PROMPT, HD), jnp.bfloat16)
        for k in range(bank):
            hit = jnp.full((PROMPT, HD), task, jnp.int32) == me * bank + k
            total = jnp.where(hit, src[k, :, head_cols(s % KVH)], total)
        sel[s * PROMPT:(s + 1) * PROMPT, :] = total

    for i in (3, 1, 2):
        loads[i].wait()
    pl.semaphore_wait(barrier, n - 1 + n_dp - 1)

    def seg_copy(src_rank, dst_rank):
        return remote(seg_ref, segs.at[src_rank], seg_s.at[dst_rank], seg_r.at[src_rank], dp, dst_rank)

    def prs_copy(src_rank, dst_rank):
        return remote(chunk(sel, dst_rank), prs.at[src_rank], prs_s.at[dst_rank], prs_r.at[src_rank], dp, dst_rank)

    def pag_copy(src_rank, dst_rank):
        return remote(chunk(pp, src_rank), chunk(pp, src_rank), pag_s.at[dst_rank], pag_r.at[src_rank], dp, dst_rank)

    def z_copy(src, blk, j):
        return remote(src, kv.at[blk * 2 + lo, j], z_s.at[blk, j], z_r.at[blk, j], dp,
                      jnp.minimum(me + 2, n - 1 - (1 - lo)))

    def x_copy(src, blk, j, side):
        return remote(src, kv.at[blk * 2 + side, j], x_s.at[blk, j], x_r.at[blk, j], dp, me + 1 - 2 * lo)

    @pl.loop(1, n)
    def _(d):
        seg_copy(me, other(d, me, n)).start()

    own = (k_ref, v_ref)

    for j in range(2):
        @pl.when(hi + 1 < n_hi)
        def _():
            z_copy(own[j], hi, j).start()

        @pl.when(lo == 0)
        def _():
            x_copy(own[j], hi, j, lo).start()

    @pl.loop(1, n)
    def _(d):
        prs_copy(me, other(d, me, n)).start()

    def queries(c):
        return jnp.concatenate([q_ref[:, head_cols(c * GROUP + g)] for g in range(GROUP)], axis=0)

    def grads(c):
        return jnp.concatenate([g_ref[:, head_cols(c * GROUP + g)] for g in range(GROUP)], axis=0)

    def wide(mask):
        return jnp.concatenate([mask] * GROUP, axis=1)

    loads[0].wait()
    q_seg = seg_ref[...]

    def column(row):
        return jnp.transpose(jnp.broadcast_to(row, (tok, tok)))

    def absorb(key_block, value_block, mask, first=False):
        mask = wide(mask)
        for c in range(KVH):
            st = dot_nt(key_block[:, head_cols(c)], queries(c)) * scale
            st = jnp.where(mask, st, -jnp.inf)
            peak = jnp.max(st, axis=0, keepdims=True)
            if not first:
                old = m_ref[c]
                peak = jnp.maximum(old, peak)
                shrink = jnp.exp(old - peak)
            w = jnp.exp(st - peak)
            total = jnp.sum(w, axis=0, keepdims=True)
            acc = dot_tn(value_block[:, head_cols(c)], w.astype(jnp.bfloat16))
            if not first:
                total = total + l_ref[c] * shrink
                acc = acc + acc_ref[c] * shrink
            m_ref[c] = peak
            l_ref[c] = total
            acc_ref[c] = acc

    order = lax.broadcasted_iota(jnp.int32, (tok, tok), 0) <= lax.broadcasted_iota(jnp.int32, (tok, tok), 1)
    absorb(k_ref, v_ref, (column(q_seg) == jnp.broadcast_to(q_seg, (tok, tok))) & order, True)

    def spread_prompt():
        def prs_add(d, total):
            src = other(d, me, n)
            prs_copy(src, me).wait_recv()
            return total + prs[src]

        mine = pl.ds(pl.multiple_of(me * rows, rows), rows)
        pp[mine, :] = lax.fori_loop(1, n, prs_add, sel[mine, :])

        @pl.loop(1, n)
        def _(d):
            pag_copy(me, other(d, me, n)).start()

    pl.when(hi == 0)(spread_prompt)

    @pl.loop(1, n)
    def _(d):
        seg_copy(other(d, me, n), me).wait_recv()

    def absorb_rank(rank):
        mask = column(segs[rank]) == jnp.broadcast_to(q_seg, (tok, tok))
        absorb(kv.at[rank, 0], kv.at[rank, 1], mask)

    def absorb_crossed(blk):
        for j in range(2):
            x_copy(own[j], blk, j, 1 - lo).wait_recv()
        absorb_rank(blk * 2 + 1 - lo)

    @pl.loop(1, hi + 1)
    def _(s):
        blk = hi - s
        for j in range(2):
            z_copy(own[j], blk, j).wait_recv()

            @pl.when(hi + 1 < n_hi)
            def _():
                z_copy(kv.at[blk * 2 + lo, j], blk, j).start()

            x_copy(kv.at[blk * 2 + lo, j], blk, j, lo).start()
        pl.when(s == jnp.minimum(hi, 2))(spread_prompt)
        absorb_rank(blk * 2 + lo)

        @pl.when(jnp.logical_or(s > 1, lo == 1))
        def _():
            absorb_crossed(blk + 1)

    @pl.loop(1, n)
    def _(d):
        pag_copy(other(d, me, n), me).wait_recv()

    loads[6].wait()
    for c in range(KVH):
        pk = pp[c * PROMPT:(c + 1) * PROMPT, :]
        pv = pp[(KVH + c) * PROMPT:(KVH + c + 1) * PROMPT, :]
        r = dot_nt(pk, queries(c)) * scale
        old = m_ref[c]
        peak = jnp.maximum(old, jnp.max(r, axis=0, keepdims=True))
        shrink = jnp.exp(old - peak)
        w = jnp.exp(r - peak)
        m_ref[c] = peak
        l_ref[c] = jnp.sum(w, axis=0, keepdims=True) + l_ref[c] * shrink
        acc_ref[c] = dot_tn(pv, w.astype(jnp.bfloat16)) + acc_ref[c] * shrink
        r_ref[c] = r
        d_ref[c] = dot_nt(pv, grads(c))

    @pl.when(jnp.logical_or(hi > 0, lo == 1))
    def _():
        absorb_crossed(0)

    def grs_copy(src_rank, dst_rank):
        return remote(chunk(part, dst_rank), grs.at[src_rank], grs_s.at[dst_rank], grs_r.at[src_rank], dp, dst_rank)

    per_slot = n // SLOTS

    def send_slot(s):
        for i in range(per_slot):
            dst = s * per_slot + i

            @pl.when(me != dst)
            def _():
                grs_copy(me, dst).start()

    for c in range(KVH):
        q = queries(c)
        g = grads(c)
        total = l_ref[c]
        att = jnp.transpose(acc_ref[c] / total).astype(jnp.bfloat16)
        for i in range(GROUP):
            att_ref[:, head_cols(c * GROUP + i)] = att[i * tok:(i + 1) * tok, :]
        delta = jnp.sum(jnp.transpose(g.astype(jnp.float32) * att.astype(jnp.float32)), axis=0, keepdims=True)
        probs = jnp.exp(r_ref[c] - (m_ref[c] + jnp.log(total)))
        score_grad = probs * (d_ref[c] - delta)
        vp = dot_nn(probs.astype(jnp.bfloat16), g)
        kp = dot_nn(score_grad.astype(jnp.bfloat16), q) * scale
        part[c * PROMPT:(c + 1) * PROMPT, :] = kp.astype(jnp.bfloat16)
        part[(KVH + c) * PROMPT:(KVH + c + 1) * PROMPT, :] = vp.astype(jnp.bfloat16)
        send_slot(c)
        send_slot(KVH + c)

    def grs_add(d, total):
        src = other(d, me, n)
        grs_copy(src, me).wait_recv()
        return total + grs[src].astype(jnp.float32)

    mine = pl.ds(pl.multiple_of(me * rows, rows), rows)
    gath[dp, mine, :] = lax.fori_loop(1, n, grs_add, part[mine, :].astype(jnp.float32)).astype(jnp.bfloat16)

    def piece(b, j):
        return gath.at[b, pl.ds(pl.multiple_of(j * rows, rows), rows)]

    def gag_copy(src_rank, dst_rank):
        return remote(piece(dp, src_rank), piece(dp, src_rank), gag_s.at[dst_rank], gag_r.at[src_rank], dp, dst_rank)

    def y_copy(src_h, dst_h, j):
        b = src_h * 2 + dl
        return remote(piece(b, j), piece(b, j), y_s.at[dst_h, j], y_r.at[src_h, j], dst_h * 2 + dl, me)

    def c_copy(h, side, j):
        b = h * 2 + side
        return remote(piece(b, j), piece(b, j), c_s.at[h, j], c_r.at[h, j], dh * 2 + 1 - dl, me)

    @pl.loop(1, n)
    def _(d):
        gag_copy(me, other(d, me, n)).start()

    def pass_on(j):
        @pl.loop(1, n_dh)
        def _(e):
            y_copy(dh, other(e, dh, n_dh), j).start()
        c_copy(dh, dl, j).start()

    pass_on(me)

    @pl.loop(1, n)
    def _(d):
        src = other(d, me, n)
        gag_copy(src, me).wait_recv()
        pass_on(src)

    @pl.loop(0, n)
    def _(d):
        src = other(d, me, n)

        @pl.loop(1, n_dh)
        def _(e):
            h = other(e, dh, n_dh)
            y_copy(h, dh, src).wait_recv()
            c_copy(h, dl, src).start()

    @pl.loop(0, n)
    def _(d):
        src = other(d, me, n)

        @pl.loop(0, n_dh)
        def _(h):
            c_copy(h, 1 - dl, src).wait_recv()

    @pl.loop(1, n)
    def _(d):
        dst = other(d, me, n)
        seg_copy(me, dst).wait_send()
        prs_copy(me, dst).wait_send()
        pag_copy(me, dst).wait_send()
        grs_copy(me, dst).wait_send()
        gag_copy(me, dst).wait_send()

    for j in range(2):
        @pl.when(lo == 0)
        def _():
            x_copy(own[j], hi, j, lo).wait_send()

        @pl.loop(0, hi)
        def _(blk):
            x_copy(own[j], blk, j, lo).wait_send()

        @pl.when(hi + 1 < n_hi)
        def _():
            @pl.loop(0, hi + 1)
            def _(blk):
                z_copy(own[j], blk, j).wait_send()

    @pl.loop(0, n)
    def _(j):
        @pl.loop(1, n_dh)
        def _(e):
            y_copy(dh, other(e, dh, n_dh), j).wait_send()

        @pl.loop(0, n_dh)
        def _(h):
            c_copy(h, dl, j).wait_send()


def finish(n_dp, task_ref, att_v, gath_v, att_out, kg_out, vg_out, kg_v, vg_v, out_s):
    bank = kg_v.shape[0]
    me = lax.axis_index("seq")
    stores = [pltpu.make_async_copy(att_v, att_out, out_s.at[2 * bank])]
    stores[0].start()
    for s in range(SLOTS):
        held, out = (kg_v, kg_out) if s < KVH else (vg_v, vg_out)
        for k in range(bank):
            total = jnp.zeros((PROMPT, HD), jnp.float32)
            for b in range(n_dp):
                hit = jnp.full((PROMPT, HD), task_ref[b], jnp.int32) == me * bank + k
                total = total + jnp.where(
                    hit, gath_v[b, s * PROMPT:(s + 1) * PROMPT, :].astype(jnp.float32), 0.0)
            held[k, :, head_cols(s % KVH)] = total
            if s % KVH == KVH - 1:
                stores.append(pltpu.make_async_copy(held.at[k], out.at[k], out_s.at[s // KVH * bank + k]))
                stores[-1].start()
    for store in stores:
        store.wait()


def shards(n, n_dp, queries, keys, values, segments, task_ids, prompt_keys, prompt_values, grad_out):
    tok = queries.shape[1]
    width = KVH * HD
    rows = SLOTS * PROMPT // n
    bank = prompt_keys.shape[0]
    bf16, f32 = jnp.bfloat16, jnp.float32
    dma = pltpu.SemaphoreType.DMA
    vmem = pl.BlockSpec(memory_space=pltpu.VMEM)
    operands = (queries[0], keys[0], values[0], segments, prompt_keys, prompt_values, grad_out[0])
    att, gath = pl.pallas_call(
        functools.partial(kernel, n, n_dp),
        out_shape=(
            pltpu.VMEM((tok, KVH * GROUP * HD), bf16),
            pltpu.VMEM((n_dp, SLOTS * PROMPT, HD), bf16),
        ),
        in_specs=[pl.BlockSpec(memory_space=pltpu.SMEM)] + [pl.BlockSpec(memory_space=pl.ANY)] * 7,
        out_specs=(vmem, vmem),
        scratch_shapes=[
            [pltpu.VMEM(a.shape, a.dtype) for a in operands],
            dma((7,)),
            pltpu.VMEM((n, 2, tok, width), bf16),
            pltpu.VMEM((n, 1, tok), jnp.int32),
            pltpu.VMEM((SLOTS * PROMPT, HD), bf16),
            pltpu.VMEM((n, rows, HD), bf16),
            pltpu.VMEM((SLOTS * PROMPT, HD), bf16),
            pltpu.VMEM((SLOTS * PROMPT, HD), bf16),
            pltpu.VMEM((n, rows, HD), bf16),
            pltpu.VMEM((KVH, 1, GROUP * tok), f32),
            pltpu.VMEM((KVH, 1, GROUP * tok), f32),
            pltpu.VMEM((KVH, HD, GROUP * tok), f32),
            pltpu.VMEM((KVH, PROMPT, GROUP * tok), f32),
            pltpu.VMEM((KVH, PROMPT, GROUP * tok), f32),
            dma((n,)), dma((n,)), dma((n,)), dma((n,)), dma((n,)), dma((n,)),
            dma((n // 2, 2)), dma((n // 2, 2)), dma((n // 2, 2)), dma((n // 2, 2)),
            dma((n,)), dma((n,)), dma((n,)), dma((n,)),
            dma((n_dp // 2, n)), dma((n_dp // 2, n)), dma((n_dp // 2, n)), dma((n_dp // 2, n)),
        ],
        compiler_params=pltpu.CompilerParams(collective_id=0, has_side_effects=True),
    )(task_ids, *operands)
    anyspace = pl.BlockSpec(memory_space=pl.ANY)
    att, kg, vg = pl.pallas_call(
        functools.partial(finish, n_dp),
        out_shape=(
            jax.ShapeDtypeStruct((tok, KVH * GROUP * HD), bf16),
            jax.ShapeDtypeStruct((bank, PROMPT, width), f32),
            jax.ShapeDtypeStruct((bank, PROMPT, width), f32),
        ),
        in_specs=[pl.BlockSpec(memory_space=pltpu.SMEM), vmem, vmem],
        out_specs=(anyspace, anyspace, anyspace),
        scratch_shapes=[
            pltpu.VMEM((bank, PROMPT, width), f32),
            pltpu.VMEM((bank, PROMPT, width), f32),
            dma((2 * bank + 1,)),
        ],
    )(task_ids, *[pltpu.with_memory_space_constraint(a, pltpu.VMEM) for a in (att, gath)])
    return att[None], kg, vg


def solution(mesh):
    n, n_dp = mesh.shape["seq"], mesh.shape["dp"]
    in_specs = (
        P("dp", "seq", None),
        P("dp", "seq", None),
        P("dp", "seq", None),
        P("dp", "seq"),
        P(),
        P("seq", None, None),
        P("seq", None, None),
        P("dp", "seq", None),
    )
    out_specs = (P("dp", "seq", None), P("seq", None, None), P("seq", None, None))
    return jax.shard_map(
        functools.partial(shards, n, n_dp), mesh=mesh, in_specs=in_specs, out_specs=out_specs, check_vma=False
    )
```

```python
import functools
import math

import jax
import jax.numpy as jnp
from jax import lax
from jax.experimental import pallas as pl
from jax.experimental.pallas import tpu as pltpu
from jax.sharding import PartitionSpec as P

KVH = 4
GROUP = 4
HD = 128
PROMPT = 128
SLOTS = 2 * KVH


def dot_nt(a, b):
    return lax.dot_general(a, b, (((1,), (1,)), ((), ())), preferred_element_type=jnp.float32)


def dot_tn(a, b):
    return lax.dot_general(a, b, (((0,), (0,)), ((), ())), preferred_element_type=jnp.float32)


def dot_nn(a, b):
    return lax.dot_general(a, b, (((1,), (0,)), ((), ())), preferred_element_type=jnp.float32)


def head_cols(c):
    return slice(c * HD, (c + 1) * HD)


def kernel(
    n, n_dp, task_ref, *refs,
):
    inputs, refs = refs[:7], refs[7:]
    att_ref, gath, held, load_s, *refs = refs
    (
    kv, segs, sel, xa, mix, w_s, w_r, sw_s, sw_r, prs, pp, part, grs, m_ref, l_ref, acc_ref, r_ref, d_ref,
    seg_s, seg_r, prs_s, prs_r, pag_s, pag_r, z_s, z_r, x_s, x_r,
    grs_s, grs_r, gag_s, gag_r, y_s, y_r, c_s, c_r,
    ) = refs
    q_ref, k_ref, v_ref, seg_ref, pk_ref, pv_ref, g_ref = held
    loads = [pltpu.make_async_copy(src, dst, load_s.at[i]) for i, (src, dst) in enumerate(zip(inputs, held))]
    for i in (4, 5, 3, 1, 2, 0, 6):
        loads[i].start()
    tok = q_ref.shape[0]
    bank = pk_ref.shape[0]
    rows = SLOTS * PROMPT // n
    n_hi = n // 2
    n_dh = n_dp // 2
    scale = 1.0 / math.sqrt(HD)
    me = lax.axis_index("seq")
    dp = lax.axis_index("dp")
    hi, lo = me // 2, me % 2
    dh, dl = dp // 2, dp % 2

    def remote(src, dst, s_sem, r_sem, to_dp, to_seq):
        return pltpu.make_async_remote_copy(
            src_ref=src, dst_ref=dst, send_sem=s_sem, recv_sem=r_sem,
            device_id=(to_dp, to_seq), device_id_type=pl.DeviceIdType.MESH,
        )

    def other(d, base, count):
        return lax.rem(base + d, count)

    def chunk(ref, j):
        return ref.at[pl.ds(pl.multiple_of(j * rows, rows), rows)]

    barrier = pltpu.get_barrier_semaphore()

    @pl.loop(1, n)
    def _(d):
        pl.semaphore_signal(barrier, inc=1, device_id=(dp, other(d, me, n)),
                            device_id_type=pl.DeviceIdType.MESH)

    @pl.loop(1, n_dp)
    def _(d):
        pl.semaphore_signal(barrier, inc=1, device_id=(other(d, dp, n_dp), me),
                            device_id_type=pl.DeviceIdType.MESH)

    for i in (4, 5):
        loads[i].wait()

    task = task_ref[dp]
    for s in range(SLOTS):
        src = pk_ref if s < KVH else pv_ref
        total = jnp.zeros((PROMPT, HD), jnp.bfloat16)
        for k in range(bank):
            hit = jnp.full((PROMPT, HD), task, jnp.int32) == me * bank + k
            total = jnp.where(hit, src[k, :, head_cols(s % KVH)], total)
        sel[s * PROMPT:(s + 1) * PROMPT, :] = total

    for i in (3, 1, 2):
        loads[i].wait()
    pl.semaphore_wait(barrier, n - 1 + n_dp - 1)

    def seg_copy(src_rank, dst_rank):
        return remote(seg_ref, segs.at[src_rank], seg_s.at[dst_rank], seg_r.at[src_rank], dp, dst_rank)

    half = SLOTS * PROMPT // 2

    def half_rows(side):
        return pl.ds(pl.multiple_of(side * half, half), half)

    def lane(h):
        return h * 2 + lo

    def swap_copy():
        return remote(sel.at[half_rows(1 - lo)], xa, sw_s.at[0], sw_r.at[0], dp, me + 1 - 2 * lo)

    def prs_copy(src_h, dst_h):
        return remote(chunk(mix, dst_h), prs.at[src_h], prs_s.at[dst_h], prs_r.at[src_h], dp, lane(dst_h))

    def pag_copy(src_h, dst_h):
        here = chunk(pp, lo * n_hi + src_h)
        return remote(here, here, pag_s.at[dst_h], pag_r.at[src_h], dp, lane(dst_h))

    def back_copy(side):
        here = pp.at[half_rows(side)]
        return remote(here, here, sw_s.at[1], sw_r.at[1], dp, me + 1 - 2 * lo)

    def z_copy(src, blk, j):
        return remote(src, kv.at[blk * 2 + lo, j], z_s.at[blk, j], z_r.at[blk, j], dp,
                      jnp.minimum(me + 2, n - 1 - (1 - lo)))

    def x_copy(src, blk, j, side):
        return remote(src, kv.at[blk * 2 + side, j], x_s.at[blk, j], x_r.at[blk, j], dp, me + 1 - 2 * lo)

    def w_copy():
        here = kv.at[1 - lo, 1]
        return remote(here, here, w_s.at[0], w_r.at[0], dp, jnp.minimum(me + 2, n - 1 - (1 - lo)))

    @pl.loop(1, n)
    def _(d):
        seg_copy(me, other(d, me, n)).start()

    swap_copy().start()
    own = (k_ref, v_ref)

    for j in range(2):
        @pl.when(hi + 1 < n_hi)
        def _():
            z_copy(own[j], hi, j).start()

        @pl.when(jnp.logical_or(lo == 0, hi == 0) if j else lo == 0)
        def _():
            x_copy(own[j], hi, j, lo).start()

    def queries(c):
        return jnp.concatenate([q_ref[:, head_cols(c * GROUP + g)] for g in range(GROUP)], axis=0)

    def grads(c):
        return jnp.concatenate([g_ref[:, head_cols(c * GROUP + g)] for g in range(GROUP)], axis=0)

    def wide(mask):
        return jnp.concatenate([mask] * GROUP, axis=1)

    loads[0].wait()
    q_seg = seg_ref[...]

    def column(row):
        return jnp.transpose(jnp.broadcast_to(row, (tok, tok)))

    def absorb(key_block, value_block, mask, first=False):
        mask = wide(mask)
        for c in range(KVH):
            st = dot_nt(key_block[:, head_cols(c)], queries(c)) * scale
            st = jnp.where(mask, st, -jnp.inf)
            peak = jnp.max(st, axis=0, keepdims=True)
            if not first:
                old = m_ref[c]
                peak = jnp.maximum(old, peak)
                shrink = jnp.exp(old - peak)
            w = jnp.exp(st - peak)
            total = jnp.sum(w, axis=0, keepdims=True)
            acc = dot_tn(value_block[:, head_cols(c)], w.astype(jnp.bfloat16))
            if not first:
                total = total + l_ref[c] * shrink
                acc = acc + acc_ref[c] * shrink
            m_ref[c] = peak
            l_ref[c] = total
            acc_ref[c] = acc

    order = lax.broadcasted_iota(jnp.int32, (tok, tok), 0) <= lax.broadcasted_iota(jnp.int32, (tok, tok), 1)
    absorb(k_ref, v_ref, (column(q_seg) == jnp.broadcast_to(q_seg, (tok, tok))) & order, True)

    swap_copy().wait_recv()
    mix[...] = sel[half_rows(lo), :] + xa[...]

    @pl.loop(1, n_hi)
    def _(d):
        prs_copy(hi, other(d, hi, n_hi)).start()

    def spread_prompt():
        def prs_add(d, total):
            src = other(d, hi, n_hi)
            prs_copy(src, hi).wait_recv()
            return total + prs[src]

        first = mix[pl.ds(pl.multiple_of(hi * rows, rows), rows), :]
        pp[pl.ds(pl.multiple_of((lo * n_hi + hi) * rows, rows), rows), :] = lax.fori_loop(1, n_hi, prs_add, first)

        @pl.loop(1, n_hi)
        def _(d):
            pag_copy(hi, other(d, hi, n_hi)).start()

    def return_prompt():
        @pl.loop(1, n_hi)
        def _(d):
            pag_copy(other(d, hi, n_hi), hi).wait_recv()

        back_copy(lo).start()

    @pl.when(hi == 0)
    def _():
        x_copy(own[1], hi, 1, 1 - lo).wait_recv()

        @pl.when(hi + 1 < n_hi)
        def _():
            w_copy().start()
        spread_prompt()

    @pl.loop(1, n)
    def _(d):
        seg_copy(other(d, me, n), me).wait_recv()

    def absorb_rank(rank):
        mask = column(segs[rank]) == jnp.broadcast_to(q_seg, (tok, tok))
        absorb(kv.at[rank, 0], kv.at[rank, 1], mask)

    def absorb_crossed(blk):
        for j in range(2):
            x_copy(own[j], blk, j, 1 - lo).wait_recv()
        absorb_rank(blk * 2 + 1 - lo)

    @pl.loop(1, hi + 1)
    def _(s):
        blk = hi - s
        pl.when(jnp.logical_and(s == hi, hi >= 3))(return_prompt)
        for j in range(2):
            z_copy(own[j], blk, j).wait_recv()

            @pl.when(hi + 1 < n_hi)
            def _():
                z_copy(kv.at[blk * 2 + lo, j], blk, j).start()

            @pl.when(blk > 0 if j else blk >= 0)
            def _():
                x_copy(kv.at[blk * 2 + lo, j], blk, j, lo).start()

        @pl.when(jnp.logical_and(s == hi, hi + 1 < n_hi))
        def _():
            w_copy().wait_recv()
            w_copy().start()
        pl.when(s == jnp.minimum(hi, 2))(spread_prompt)
        absorb_rank(blk * 2 + lo)

        @pl.when(jnp.logical_or(s > 1, lo == 1))
        def _():
            absorb_crossed(blk + 1)

    pl.when(hi < 3)(return_prompt)
    back_copy(1 - lo).wait_recv()

    loads[6].wait()
    for c in range(KVH):
        pk = pp[c * PROMPT:(c + 1) * PROMPT, :]
        pv = pp[(KVH + c) * PROMPT:(KVH + c + 1) * PROMPT, :]
        r = dot_nt(pk, queries(c)) * scale
        old = m_ref[c]
        peak = jnp.maximum(old, jnp.max(r, axis=0, keepdims=True))
        shrink = jnp.exp(old - peak)
        w = jnp.exp(r - peak)
        m_ref[c] = peak
        l_ref[c] = jnp.sum(w, axis=0, keepdims=True) + l_ref[c] * shrink
        acc_ref[c] = dot_tn(pv, w.astype(jnp.bfloat16)) + acc_ref[c] * shrink
        r_ref[c] = r
        d_ref[c] = dot_nt(pv, grads(c))

    @pl.when(jnp.logical_and(hi > 0, hi + 1 == n_hi))
    def _():
        w_copy().wait_recv()

    @pl.when(jnp.logical_or(hi > 0, lo == 1))
    def _():
        x_copy(own[0], 0, 0, 1 - lo).wait_recv()
        absorb_rank(1 - lo)

    def grs_copy(src_rank, dst_rank):
        return remote(chunk(part, dst_rank), grs.at[src_rank], grs_s.at[dst_rank], grs_r.at[src_rank], dp, dst_rank)

    per_slot = n // SLOTS

    def send_slot(s):
        for i in range(per_slot):
            dst = s * per_slot + i

            @pl.when(me != dst)
            def _():
                grs_copy(me, dst).start()

    for c in range(KVH):
        q = queries(c)
        g = grads(c)
        total = l_ref[c]
        att = jnp.transpose(acc_ref[c] / total).astype(jnp.bfloat16)
        for i in range(GROUP):
            att_ref[:, head_cols(c * GROUP + i)] = att[i * tok:(i + 1) * tok, :]
        delta = jnp.sum(jnp.transpose(g.astype(jnp.float32) * att.astype(jnp.float32)), axis=0, keepdims=True)
        probs = jnp.exp(r_ref[c] - (m_ref[c] + jnp.log(total)))
        score_grad = probs * (d_ref[c] - delta)
        vp = dot_nn(probs.astype(jnp.bfloat16), g)
        kp = dot_nn(score_grad.astype(jnp.bfloat16), q) * scale
        part[c * PROMPT:(c + 1) * PROMPT, :] = kp.astype(jnp.bfloat16)
        part[(KVH + c) * PROMPT:(KVH + c + 1) * PROMPT, :] = vp.astype(jnp.bfloat16)
        send_slot(c)
        send_slot(KVH + c)

    def grs_add(d, total):
        src = other(d, me, n)
        grs_copy(src, me).wait_recv()
        return total + grs[src].astype(jnp.float32)

    mine = pl.ds(pl.multiple_of(me * rows, rows), rows)
    gath[dp, mine, :] = lax.fori_loop(1, n, grs_add, part[mine, :].astype(jnp.float32)).astype(jnp.bfloat16)

    def piece(b, j):
        return gath.at[b, pl.ds(pl.multiple_of(j * rows, rows), rows)]

    def gag_copy(src_rank, dst_rank):
        return remote(piece(dp, src_rank), piece(dp, src_rank), gag_s.at[dst_rank], gag_r.at[src_rank], dp, dst_rank)

    def y_copy(src_h, dst_h, j):
        b = src_h * 2 + dl
        return remote(piece(b, j), piece(b, j), y_s.at[dst_h, j], y_r.at[src_h, j], dst_h * 2 + dl, me)

    def c_copy(h, side, j):
        b = h * 2 + side
        return remote(piece(b, j), piece(b, j), c_s.at[h, j], c_r.at[h, j], dh * 2 + 1 - dl, me)

    @pl.loop(1, n)
    def _(d):
        gag_copy(me, other(d, me, n)).start()

    def pass_on(j):
        @pl.loop(1, n_dh)
        def _(e):
            y_copy(dh, other(e, dh, n_dh), j).start()
        c_copy(dh, dl, j).start()

    pass_on(me)

    @pl.loop(1, n)
    def _(d):
        src = other(d, me, n)
        gag_copy(src, me).wait_recv()
        pass_on(src)

    @pl.loop(0, n)
    def _(d):
        src = other(d, me, n)

        @pl.loop(1, n_dh)
        def _(e):
            h = other(e, dh, n_dh)
            y_copy(h, dh, src).wait_recv()
            c_copy(h, dl, src).start()

    @pl.loop(0, n)
    def _(d):
        src = other(d, me, n)

        @pl.loop(0, n_dh)
        def _(h):
            c_copy(h, 1 - dl, src).wait_recv()

    @pl.loop(1, n)
    def _(d):
        dst = other(d, me, n)
        seg_copy(me, dst).wait_send()
        grs_copy(me, dst).wait_send()
        gag_copy(me, dst).wait_send()

    swap_copy().wait_send()
    pl.when(hi + 1 < n_hi)(lambda: w_copy().wait_send())
    back_copy(lo).wait_send()

    @pl.loop(1, n_hi)
    def _(d):
        dst = other(d, hi, n_hi)
        prs_copy(hi, dst).wait_send()
        pag_copy(hi, dst).wait_send()

    for j in range(2):
        @pl.when(jnp.logical_or(lo == 0, hi == 0) if j else lo == 0)
        def _():
            x_copy(own[j], hi, j, lo).wait_send()

        @pl.loop(j, hi)
        def _(blk):
            x_copy(own[j], blk, j, lo).wait_send()

        @pl.when(hi + 1 < n_hi)
        def _():
            @pl.loop(0, hi + 1)
            def _(blk):
                z_copy(own[j], blk, j).wait_send()

    @pl.loop(0, n)
    def _(j):
        @pl.loop(1, n_dh)
        def _(e):
            y_copy(dh, other(e, dh, n_dh), j).wait_send()

        @pl.loop(0, n_dh)
        def _(h):
            c_copy(h, dl, j).wait_send()


def finish(n_dp, task_ref, att_v, gath_v, att_out, kg_out, vg_out, kg_v, vg_v, out_s):
    bank = kg_v.shape[0]
    me = lax.axis_index("seq")
    stores = [pltpu.make_async_copy(att_v, att_out, out_s.at[2 * bank])]
    stores[0].start()
    for s in range(SLOTS):
        held, out = (kg_v, kg_out) if s < KVH else (vg_v, vg_out)
        for k in range(bank):
            total = jnp.zeros((PROMPT, HD), jnp.float32)
            for b in range(n_dp):
                hit = jnp.full((PROMPT, HD), task_ref[b], jnp.int32) == me * bank + k
                total = total + jnp.where(
                    hit, gath_v[b, s * PROMPT:(s + 1) * PROMPT, :].astype(jnp.float32), 0.0)
            held[k, :, head_cols(s % KVH)] = total
            if s % KVH == KVH - 1:
                stores.append(pltpu.make_async_copy(held.at[k], out.at[k], out_s.at[s // KVH * bank + k]))
                stores[-1].start()
    for store in stores:
        store.wait()


def shards(n, n_dp, queries, keys, values, segments, task_ids, prompt_keys, prompt_values, grad_out):
    tok = queries.shape[1]
    width = KVH * HD
    rows = SLOTS * PROMPT // n
    bank = prompt_keys.shape[0]
    bf16, f32 = jnp.bfloat16, jnp.float32
    dma = pltpu.SemaphoreType.DMA
    vmem = pl.BlockSpec(memory_space=pltpu.VMEM)
    operands = (queries[0], keys[0], values[0], segments, prompt_keys, prompt_values, grad_out[0])
    att, gath = pl.pallas_call(
        functools.partial(kernel, n, n_dp),
        out_shape=(
            pltpu.VMEM((tok, KVH * GROUP * HD), bf16),
            pltpu.VMEM((n_dp, SLOTS * PROMPT, HD), bf16),
        ),
        in_specs=[pl.BlockSpec(memory_space=pltpu.SMEM)] + [pl.BlockSpec(memory_space=pl.ANY)] * 7,
        out_specs=(vmem, vmem),
        scratch_shapes=[
            [pltpu.VMEM(a.shape, a.dtype) for a in operands],
            dma((7,)),
            pltpu.VMEM((n, 2, tok, width), bf16),
            pltpu.VMEM((n, 1, tok), jnp.int32),
            pltpu.VMEM((SLOTS * PROMPT, HD), bf16),
            pltpu.VMEM((SLOTS * PROMPT // 2, HD), bf16),
            pltpu.VMEM((SLOTS * PROMPT // 2, HD), bf16),
            dma((1,)), dma((1,)), dma((2,)), dma((2,)),
            pltpu.VMEM((n // 2, rows, HD), bf16),
            pltpu.VMEM((SLOTS * PROMPT, HD), bf16),
            pltpu.VMEM((SLOTS * PROMPT, HD), bf16),
            pltpu.VMEM((n, rows, HD), bf16),
            pltpu.VMEM((KVH, 1, GROUP * tok), f32),
            pltpu.VMEM((KVH, 1, GROUP * tok), f32),
            pltpu.VMEM((KVH, HD, GROUP * tok), f32),
            pltpu.VMEM((KVH, PROMPT, GROUP * tok), f32),
            pltpu.VMEM((KVH, PROMPT, GROUP * tok), f32),
            dma((n,)), dma((n,)), dma((n // 2,)), dma((n // 2,)), dma((n // 2,)), dma((n // 2,)),
            dma((n // 2, 2)), dma((n // 2, 2)), dma((n // 2, 2)), dma((n // 2, 2)),
            dma((n,)), dma((n,)), dma((n,)), dma((n,)),
            dma((n_dp // 2, n)), dma((n_dp // 2, n)), dma((n_dp // 2, n)), dma((n_dp // 2, n)),
        ],
        compiler_params=pltpu.CompilerParams(collective_id=0, has_side_effects=True),
    )(task_ids, *operands)
    anyspace = pl.BlockSpec(memory_space=pl.ANY)
    att, kg, vg = pl.pallas_call(
        functools.partial(finish, n_dp),
        out_shape=(
            jax.ShapeDtypeStruct((tok, KVH * GROUP * HD), bf16),
            jax.ShapeDtypeStruct((bank, PROMPT, width), f32),
            jax.ShapeDtypeStruct((bank, PROMPT, width), f32),
        ),
        in_specs=[pl.BlockSpec(memory_space=pltpu.SMEM), vmem, vmem],
        out_specs=(anyspace, anyspace, anyspace),
        scratch_shapes=[
            pltpu.VMEM((bank, PROMPT, width), f32),
            pltpu.VMEM((bank, PROMPT, width), f32),
            dma((2 * bank + 1,)),
        ],
    )(task_ids, *[pltpu.with_memory_space_constraint(a, pltpu.VMEM) for a in (att, gath)])
    return att[None], kg, vg


def solution(mesh):
    n, n_dp = mesh.shape["seq"], mesh.shape["dp"]
    in_specs = (
        P("dp", "seq", None),
        P("dp", "seq", None),
        P("dp", "seq", None),
        P("dp", "seq"),
        P(),
        P("seq", None, None),
        P("seq", None, None),
        P("dp", "seq", None),
    )
    out_specs = (P("dp", "seq", None), P("seq", None, None), P("seq", None, None))
    return jax.shard_map(
        functools.partial(shards, n, n_dp), mesh=mesh, in_specs=in_specs, out_specs=out_specs, check_vma=False
    )
```

```python
import functools
import math

import jax
import jax.numpy as jnp
from jax import lax
from jax.experimental import pallas as pl
from jax.experimental.pallas import tpu as pltpu
from jax.sharding import PartitionSpec as P

KVH = 4
GROUP = 4
HD = 128
PROMPT = 128
SLOTS = 2 * KVH


def dot_nt(a, b):
    return lax.dot_general(a, b, (((1,), (1,)), ((), ())), preferred_element_type=jnp.float32)


def dot_tn(a, b):
    return lax.dot_general(a, b, (((0,), (0,)), ((), ())), preferred_element_type=jnp.float32)


def dot_nn(a, b):
    return lax.dot_general(a, b, (((1,), (0,)), ((), ())), preferred_element_type=jnp.float32)


def head_cols(c):
    return slice(c * HD, (c + 1) * HD)


def kernel(
    n, n_dp, task_ref, *refs,
):
    inputs, refs = refs[:7], refs[7:]
    att_ref, gath, held, load_s, *refs = refs
    (
    kv, segs, sel, near_ref, xa, mix, w_s, w_r, sw_s, sw_r, prs, pp, part, grs, m_ref, l_ref, acc_ref, r_ref, d_ref,
    seg_s, seg_r, prs_s, prs_r, pag_s, pag_r, z_s, z_r, x_s, x_r,
    grs_s, grs_r, gag_s, gag_r, y_s, y_r, c_s, c_r,
    ) = refs
    q_ref, k_ref, v_ref, seg_ref, pk_ref, pv_ref, g_ref = held
    loads = [pltpu.make_async_copy(src, dst, load_s.at[i]) for i, (src, dst) in enumerate(zip(inputs, held))]
    for i in (4, 5, 3, 1, 2, 0, 6):
        loads[i].start()
    tok = q_ref.shape[0]
    bank = pk_ref.shape[0]
    rows = SLOTS * PROMPT // n
    n_hi = n // 2
    n_dh = n_dp // 2
    scale = 1.0 / math.sqrt(HD)
    me = lax.axis_index("seq")
    dp = lax.axis_index("dp")
    hi, lo = me // 2, me % 2
    dh, dl = dp // 2, dp % 2

    def remote(src, dst, s_sem, r_sem, to_dp, to_seq):
        return pltpu.make_async_remote_copy(
            src_ref=src, dst_ref=dst, send_sem=s_sem, recv_sem=r_sem,
            device_id=(to_dp, to_seq), device_id_type=pl.DeviceIdType.MESH,
        )

    def other(d, base, count):
        return lax.rem(base + d, count)

    def chunk(ref, j):
        return ref.at[pl.ds(pl.multiple_of(j * rows, rows), rows)]

    barrier = pltpu.get_barrier_semaphore()

    @pl.loop(1, n)
    def _(d):
        pl.semaphore_signal(barrier, inc=1, device_id=(dp, other(d, me, n)),
                            device_id_type=pl.DeviceIdType.MESH)

    @pl.loop(1, n_dp)
    def _(d):
        pl.semaphore_signal(barrier, inc=1, device_id=(other(d, dp, n_dp), me),
                            device_id_type=pl.DeviceIdType.MESH)

    for i in (4, 5):
        loads[i].wait()

    task = task_ref[dp]
    for s in range(SLOTS):
        src = pk_ref if s < KVH else pv_ref
        total = jnp.zeros((PROMPT, HD), jnp.bfloat16)
        for k in range(bank):
            hit = jnp.full((PROMPT, HD), task, jnp.int32) == me * bank + k
            total = jnp.where(hit, src[k, :, head_cols(s % KVH)], total)
        sel[s * PROMPT:(s + 1) * PROMPT, :] = total

    for i in (3, 1, 2):
        loads[i].wait()
    pl.semaphore_wait(barrier, n - 1 + n_dp - 1)

    def seg_copy(src_rank, dst_rank):
        return remote(seg_ref, segs.at[src_rank], seg_s.at[dst_rank], seg_r.at[src_rank], dp, dst_rank)

    half = SLOTS * PROMPT // 2

    def half_rows(side):
        return pl.ds(pl.multiple_of(side * half, half), half)

    def lane(h):
        return h * 2 + lo

    def swap_copy():
        return remote(sel.at[half_rows(1 - lo)], xa, sw_s.at[0], sw_r.at[0], dp, me + 1 - 2 * lo)

    def prs_copy(src_h, dst_h):
        return remote(chunk(mix, dst_h), prs.at[src_h], prs_s.at[dst_h], prs_r.at[src_h], dp, lane(dst_h))

    def pag_copy(src_h, dst_h):
        here = chunk(pp, lo * n_hi + src_h)
        return remote(here, here, pag_s.at[dst_h], pag_r.at[src_h], dp, lane(dst_h))

    def back_copy(side):
        here = pp.at[half_rows(side)]
        return remote(here, here, sw_s.at[1], sw_r.at[1], dp, me + 1 - 2 * lo)

    def z_copy(src, blk, j):
        return remote(src, kv.at[blk * 2 + lo, j], z_s.at[blk, j], z_r.at[blk, j], dp,
                      jnp.minimum(me + 2, n - 1 - (1 - lo)))

    def x_copy(src, blk, j, side):
        return remote(src, kv.at[blk * 2 + side, j], x_s.at[blk, j], x_r.at[blk, j], dp, me + 1 - 2 * lo)

    def w_copy():
        here = kv.at[1 - lo, 1]
        return remote(here, here, w_s.at[0], w_r.at[0], dp, jnp.minimum(me + 2, n - 1 - (1 - lo)))

    @pl.loop(1, n)
    def _(d):
        seg_copy(me, other(d, me, n)).start()

    swap_copy().start()
    own = (k_ref, v_ref)

    for j in range(2):
        @pl.when(hi + 1 < n_hi)
        def _():
            z_copy(own[j], hi, j).start()

        @pl.when(jnp.logical_or(lo == 0, hi == 0) if j else lo == 0)
        def _():
            x_copy(own[j], hi, j, lo).start()

    def queries(c):
        return jnp.concatenate([q_ref[:, head_cols(c * GROUP + g)] for g in range(GROUP)], axis=0)

    def grads(c):
        return jnp.concatenate([g_ref[:, head_cols(c * GROUP + g)] for g in range(GROUP)], axis=0)

    def wide(mask):
        return jnp.concatenate([mask] * GROUP, axis=1)

    loads[0].wait()
    q_seg = seg_ref[...]

    def column(row):
        return jnp.transpose(jnp.broadcast_to(row, (tok, tok)))

    def absorb(key_block, value_block, mask, first=False, heads=range(KVH)):
        mask = wide(mask)
        for c in heads:
            st = dot_nt(key_block[:, head_cols(c)], queries(c)) * scale
            st = jnp.where(mask, st, -jnp.inf)
            peak = jnp.max(st, axis=0, keepdims=True)
            if not first:
                old = m_ref[c]
                peak = jnp.maximum(old, peak)
                shrink = jnp.exp(old - peak)
            w = jnp.exp(st - peak)
            total = jnp.sum(w, axis=0, keepdims=True)
            acc = dot_tn(value_block[:, head_cols(c)], w.astype(jnp.bfloat16))
            if not first:
                total = total + l_ref[c] * shrink
                acc = acc + acc_ref[c] * shrink
            m_ref[c] = peak
            l_ref[c] = total
            acc_ref[c] = acc

    order = lax.broadcasted_iota(jnp.int32, (tok, tok), 0) <= lax.broadcasted_iota(jnp.int32, (tok, tok), 1)
    absorb(k_ref, v_ref, (column(q_seg) == jnp.broadcast_to(q_seg, (tok, tok))) & order, True)

    swap_copy().wait_recv()
    mix[...] = sel[half_rows(lo), :] + xa[...]

    @pl.loop(1, n_hi)
    def _(d):
        prs_copy(hi, other(d, hi, n_hi)).start()

    def spread_prompt():
        def prs_add(d, total):
            src = other(d, hi, n_hi)
            prs_copy(src, hi).wait_recv()
            return total + prs[src]

        first = mix[pl.ds(pl.multiple_of(hi * rows, rows), rows), :]
        pp[pl.ds(pl.multiple_of((lo * n_hi + hi) * rows, rows), rows), :] = lax.fori_loop(1, n_hi, prs_add, first)

        @pl.loop(1, n_hi)
        def _(d):
            pag_copy(hi, other(d, hi, n_hi)).start()

    def return_prompt():
        @pl.loop(1, n_hi)
        def _(d):
            pag_copy(other(d, hi, n_hi), hi).wait_recv()

        back_copy(lo).start()

    @pl.when(hi == 0)
    def _():
        x_copy(own[1], hi, 1, 1 - lo).wait_recv()

        @pl.when(hi + 1 < n_hi)
        def _():
            w_copy().start()
        spread_prompt()

    @pl.loop(1, n)
    def _(d):
        seg_copy(other(d, me, n), me).wait_recv()

    def absorb_rank(rank):
        mask = column(segs[rank]) == jnp.broadcast_to(q_seg, (tok, tok))
        absorb(kv.at[rank, 0], kv.at[rank, 1], mask)

    def absorb_crossed(blk):
        for j in range(2):
            x_copy(own[j], blk, j, 1 - lo).wait_recv()
        absorb_rank(blk * 2 + 1 - lo)

    @pl.loop(1, hi + 1)
    def _(s):
        blk = hi - s
        pl.when(jnp.logical_and(s == hi, hi >= 3))(return_prompt)
        for j in range(2):
            z_copy(own[j], blk, j).wait_recv()

            @pl.when(hi + 1 < n_hi)
            def _():
                z_copy(kv.at[blk * 2 + lo, j], blk, j).start()

            @pl.when(blk > 0 if j else blk >= 0)
            def _():
                x_copy(kv.at[blk * 2 + lo, j], blk, j, lo).start()

        @pl.when(jnp.logical_and(s == hi, hi + 1 < n_hi))
        def _():
            w_copy().wait_recv()
            w_copy().start()
        pl.when(s == jnp.minimum(hi, 2))(spread_prompt)
        absorb_rank(blk * 2 + lo)

        @pl.when(jnp.logical_or(s > 1, lo == 1))
        def _():
            absorb_crossed(blk + 1)

    pl.when(hi < 3)(return_prompt)
    back_copy(1 - lo).wait_recv()

    loads[6].wait()
    for c in range(KVH):
        pk = pp[c * PROMPT:(c + 1) * PROMPT, :]
        pv = pp[(KVH + c) * PROMPT:(KVH + c + 1) * PROMPT, :]
        r = dot_nt(pk, queries(c)) * scale
        old = m_ref[c]
        peak = jnp.maximum(old, jnp.max(r, axis=0, keepdims=True))
        shrink = jnp.exp(old - peak)
        w = jnp.exp(r - peak)
        m_ref[c] = peak
        l_ref[c] = jnp.sum(w, axis=0, keepdims=True) + l_ref[c] * shrink
        acc_ref[c] = dot_tn(pv, w.astype(jnp.bfloat16)) + acc_ref[c] * shrink
        r_ref[c] = r
        d_ref[c] = dot_nt(pv, grads(c))

    @pl.when(jnp.logical_and(hi > 0, hi + 1 == n_hi))
    def _():
        w_copy().wait_recv()

    crossed = jnp.logical_or(hi > 0, lo == 1)

    @pl.when(crossed)
    def _():
        near_ref[...] = column(segs[1 - lo])
        x_copy(own[0], 0, 0, 1 - lo).wait_recv()

    def grs_copy(src_rank, dst_rank):
        return remote(chunk(part, dst_rank), grs.at[src_rank], grs_s.at[dst_rank], grs_r.at[src_rank], dp, dst_rank)

    per_slot = n // SLOTS

    def send_slot(s):
        for i in range(per_slot):
            dst = s * per_slot + i

            @pl.when(me != dst)
            def _():
                grs_copy(me, dst).start()

    for c in range(KVH):
        @pl.when(crossed)
        def _():
            mask = near_ref[...] == jnp.broadcast_to(q_seg, (tok, tok))
            absorb(kv.at[1 - lo, 0], kv.at[1 - lo, 1], mask, heads=(c,))

        q = queries(c)
        g = grads(c)
        total = l_ref[c]
        att = jnp.transpose(acc_ref[c] / total).astype(jnp.bfloat16)
        for i in range(GROUP):
            att_ref[:, head_cols(c * GROUP + i)] = att[i * tok:(i + 1) * tok, :]
        delta = jnp.sum(jnp.transpose(g.astype(jnp.float32) * att.astype(jnp.float32)), axis=0, keepdims=True)
        probs = jnp.exp(r_ref[c] - (m_ref[c] + jnp.log(total)))
        score_grad = probs * (d_ref[c] - delta)
        vp = dot_nn(probs.astype(jnp.bfloat16), g)
        kp = dot_nn(score_grad.astype(jnp.bfloat16), q) * scale
        part[c * PROMPT:(c + 1) * PROMPT, :] = kp.astype(jnp.bfloat16)
        part[(KVH + c) * PROMPT:(KVH + c + 1) * PROMPT, :] = vp.astype(jnp.bfloat16)
        send_slot(c)
        send_slot(KVH + c)

    def grs_add(d, total):
        src = other(d, me, n)
        grs_copy(src, me).wait_recv()
        return total + grs[src].astype(jnp.float32)

    mine = pl.ds(pl.multiple_of(me * rows, rows), rows)
    gath[dp, mine, :] = lax.fori_loop(1, n, grs_add, part[mine, :].astype(jnp.float32)).astype(jnp.bfloat16)

    def piece(b, j):
        return gath.at[b, pl.ds(pl.multiple_of(j * rows, rows), rows)]

    def gag_copy(src_rank, dst_rank):
        return remote(piece(dp, src_rank), piece(dp, src_rank), gag_s.at[dst_rank], gag_r.at[src_rank], dp, dst_rank)

    def y_copy(src_h, dst_h, j):
        b = src_h * 2 + dl
        return remote(piece(b, j), piece(b, j), y_s.at[dst_h, j], y_r.at[src_h, j], dst_h * 2 + dl, me)

    def c_copy(h, side, j):
        b = h * 2 + side
        return remote(piece(b, j), piece(b, j), c_s.at[h, j], c_r.at[h, j], dh * 2 + 1 - dl, me)

    @pl.loop(1, n)
    def _(d):
        gag_copy(me, other(d, me, n)).start()

    def pass_on(j):
        @pl.loop(1, n_dh)
        def _(e):
            y_copy(dh, other(e, dh, n_dh), j).start()
        c_copy(dh, dl, j).start()

    pass_on(me)

    @pl.loop(1, n)
    def _(d):
        src = other(d, me, n)
        gag_copy(src, me).wait_recv()
        pass_on(src)

    @pl.loop(0, n)
    def _(d):
        src = other(d, me, n)

        @pl.loop(1, n_dh)
        def _(e):
            h = other(e, dh, n_dh)
            y_copy(h, dh, src).wait_recv()
            c_copy(h, dl, src).start()

    @pl.loop(0, n)
    def _(d):
        src = other(d, me, n)

        @pl.loop(0, n_dh)
        def _(h):
            c_copy(h, 1 - dl, src).wait_recv()

    @pl.loop(1, n)
    def _(d):
        dst = other(d, me, n)
        seg_copy(me, dst).wait_send()
        grs_copy(me, dst).wait_send()
        gag_copy(me, dst).wait_send()

    swap_copy().wait_send()
    pl.when(hi + 1 < n_hi)(lambda: w_copy().wait_send())
    back_copy(lo).wait_send()

    @pl.loop(1, n_hi)
    def _(d):
        dst = other(d, hi, n_hi)
        prs_copy(hi, dst).wait_send()
        pag_copy(hi, dst).wait_send()

    for j in range(2):
        @pl.when(jnp.logical_or(lo == 0, hi == 0) if j else lo == 0)
        def _():
            x_copy(own[j], hi, j, lo).wait_send()

        @pl.loop(j, hi)
        def _(blk):
            x_copy(own[j], blk, j, lo).wait_send()

        @pl.when(hi + 1 < n_hi)
        def _():
            @pl.loop(0, hi + 1)
            def _(blk):
                z_copy(own[j], blk, j).wait_send()

    @pl.loop(0, n)
    def _(j):
        @pl.loop(1, n_dh)
        def _(e):
            y_copy(dh, other(e, dh, n_dh), j).wait_send()

        @pl.loop(0, n_dh)
        def _(h):
            c_copy(h, dl, j).wait_send()


def finish(n_dp, task_ref, att_v, gath_v, att_out, kg_out, vg_out, kg_v, vg_v, out_s):
    bank = kg_v.shape[0]
    me = lax.axis_index("seq")
    stores = [pltpu.make_async_copy(att_v, att_out, out_s.at[2 * bank])]
    stores[0].start()
    for s in range(SLOTS):
        held, out = (kg_v, kg_out) if s < KVH else (vg_v, vg_out)
        for k in range(bank):
            total = jnp.zeros((PROMPT, HD), jnp.float32)
            for b in range(n_dp):
                hit = jnp.full((PROMPT, HD), task_ref[b], jnp.int32) == me * bank + k
                total = total + jnp.where(
                    hit, gath_v[b, s * PROMPT:(s + 1) * PROMPT, :].astype(jnp.float32), 0.0)
            held[k, :, head_cols(s % KVH)] = total
            if s % KVH == KVH - 1:
                stores.append(pltpu.make_async_copy(held.at[k], out.at[k], out_s.at[s // KVH * bank + k]))
                stores[-1].start()
    for store in stores:
        store.wait()


def shards(n, n_dp, queries, keys, values, segments, task_ids, prompt_keys, prompt_values, grad_out):
    tok = queries.shape[1]
    width = KVH * HD
    rows = SLOTS * PROMPT // n
    bank = prompt_keys.shape[0]
    bf16, f32 = jnp.bfloat16, jnp.float32
    dma = pltpu.SemaphoreType.DMA
    vmem = pl.BlockSpec(memory_space=pltpu.VMEM)
    operands = (queries[0], keys[0], values[0], segments, prompt_keys, prompt_values, grad_out[0])
    att, gath = pl.pallas_call(
        functools.partial(kernel, n, n_dp),
        out_shape=(
            pltpu.VMEM((tok, KVH * GROUP * HD), bf16),
            pltpu.VMEM((n_dp, SLOTS * PROMPT, HD), bf16),
        ),
        in_specs=[pl.BlockSpec(memory_space=pltpu.SMEM)] + [pl.BlockSpec(memory_space=pl.ANY)] * 7,
        out_specs=(vmem, vmem),
        scratch_shapes=[
            [pltpu.VMEM(a.shape, a.dtype) for a in operands],
            dma((7,)),
            pltpu.VMEM((n, 2, tok, width), bf16),
            pltpu.VMEM((n, 1, tok), jnp.int32),
            pltpu.VMEM((SLOTS * PROMPT, HD), bf16),
            pltpu.VMEM((tok, tok), jnp.int32),
            pltpu.VMEM((SLOTS * PROMPT // 2, HD), bf16),
            pltpu.VMEM((SLOTS * PROMPT // 2, HD), bf16),
            dma((1,)), dma((1,)), dma((2,)), dma((2,)),
            pltpu.VMEM((n // 2, rows, HD), bf16),
            pltpu.VMEM((SLOTS * PROMPT, HD), bf16),
            pltpu.VMEM((SLOTS * PROMPT, HD), bf16),
            pltpu.VMEM((n, rows, HD), bf16),
            pltpu.VMEM((KVH, 1, GROUP * tok), f32),
            pltpu.VMEM((KVH, 1, GROUP * tok), f32),
            pltpu.VMEM((KVH, HD, GROUP * tok), f32),
            pltpu.VMEM((KVH, PROMPT, GROUP * tok), f32),
            pltpu.VMEM((KVH, PROMPT, GROUP * tok), f32),
            dma((n,)), dma((n,)), dma((n // 2,)), dma((n // 2,)), dma((n // 2,)), dma((n // 2,)),
            dma((n // 2, 2)), dma((n // 2, 2)), dma((n // 2, 2)), dma((n // 2, 2)),
            dma((n,)), dma((n,)), dma((n,)), dma((n,)),
            dma((n_dp // 2, n)), dma((n_dp // 2, n)), dma((n_dp // 2, n)), dma((n_dp // 2, n)),
        ],
        compiler_params=pltpu.CompilerParams(collective_id=0, has_side_effects=True),
    )(task_ids, *operands)
    anyspace = pl.BlockSpec(memory_space=pl.ANY)
    att, kg, vg = pl.pallas_call(
        functools.partial(finish, n_dp),
        out_shape=(
            jax.ShapeDtypeStruct((tok, KVH * GROUP * HD), bf16),
            jax.ShapeDtypeStruct((bank, PROMPT, width), f32),
            jax.ShapeDtypeStruct((bank, PROMPT, width), f32),
        ),
        in_specs=[pl.BlockSpec(memory_space=pltpu.SMEM), vmem, vmem],
        out_specs=(anyspace, anyspace, anyspace),
        scratch_shapes=[
            pltpu.VMEM((bank, PROMPT, width), f32),
            pltpu.VMEM((bank, PROMPT, width), f32),
            dma((2 * bank + 1,)),
        ],
    )(task_ids, *[pltpu.with_memory_space_constraint(a, pltpu.VMEM) for a in (att, gath)])
    return att[None], kg, vg


def solution(mesh):
    n, n_dp = mesh.shape["seq"], mesh.shape["dp"]
    in_specs = (
        P("dp", "seq", None),
        P("dp", "seq", None),
        P("dp", "seq", None),
        P("dp", "seq"),
        P(),
        P("seq", None, None),
        P("seq", None, None),
        P("dp", "seq", None),
    )
    out_specs = (P("dp", "seq", None), P("seq", None, None), P("seq", None, None))
    return jax.shard_map(
        functools.partial(shards, n, n_dp), mesh=mesh, in_specs=in_specs, out_specs=out_specs, check_vma=False
    )
```

```python
import functools
import math

import jax
import jax.numpy as jnp
from jax import lax
from jax.experimental import pallas as pl
from jax.experimental.pallas import tpu as pltpu
from jax.sharding import PartitionSpec as P

KVH = 4
GROUP = 4
HD = 128
PROMPT = 128
SLOTS = 2 * KVH


def dot_nt(a, b):
    return lax.dot_general(a, b, (((1,), (1,)), ((), ())), preferred_element_type=jnp.float32)


def dot_tn(a, b):
    return lax.dot_general(a, b, (((0,), (0,)), ((), ())), preferred_element_type=jnp.float32)


def dot_nn(a, b):
    return lax.dot_general(a, b, (((1,), (0,)), ((), ())), preferred_element_type=jnp.float32)


def head_cols(c):
    return slice(c * HD, (c + 1) * HD)


def kernel(
    n, n_dp, task_ref, *refs,
):
    inputs, refs = refs[:7], refs[7:]
    att_ref, gath, held, load_s, *refs = refs
    (
    kv, segs, sel, near_ref, xa, mix, w_s, w_r, sw_s, sw_r, prs, pp, part, grs, m_ref, l_ref, acc_ref, r_ref, d_ref,
    seg_s, seg_r, prs_s, prs_r, pag_s, pag_r, z_s, z_r, x_s, x_r,
    grs_s, grs_r, gag_s, gag_r, y_s, y_r, c_s, c_r,
    ) = refs
    q_ref, k_ref, v_ref, seg_ref, pk_ref, pv_ref, g_ref = held
    loads = [pltpu.make_async_copy(src, dst, load_s.at[i]) for i, (src, dst) in enumerate(zip(inputs, held))]
    for i in (4, 5, 3, 1, 2, 0, 6):
        loads[i].start()
    tok = q_ref.shape[0]
    bank = pk_ref.shape[0]
    rows = SLOTS * PROMPT // n
    n_hi = n // 2
    n_dh = n_dp // 2
    scale = 1.0 / math.sqrt(HD)
    me = lax.axis_index("seq")
    dp = lax.axis_index("dp")
    hi, lo = me // 2, me % 2
    dh, dl = dp // 2, dp % 2

    def remote(src, dst, s_sem, r_sem, to_dp, to_seq):
        return pltpu.make_async_remote_copy(
            src_ref=src, dst_ref=dst, send_sem=s_sem, recv_sem=r_sem,
            device_id=(to_dp, to_seq), device_id_type=pl.DeviceIdType.MESH,
        )

    def other(d, base, count):
        return lax.rem(base + d, count)

    def chunk(ref, j):
        return ref.at[pl.ds(pl.multiple_of(j * rows, rows), rows)]

    barrier = pltpu.get_barrier_semaphore()

    @pl.loop(1, n)
    def _(d):
        pl.semaphore_signal(barrier, inc=1, device_id=(dp, other(d, me, n)),
                            device_id_type=pl.DeviceIdType.MESH)

    @pl.loop(1, n_dp)
    def _(d):
        pl.semaphore_signal(barrier, inc=1, device_id=(other(d, dp, n_dp), me),
                            device_id_type=pl.DeviceIdType.MESH)

    for i in (4, 5):
        loads[i].wait()

    task = task_ref[dp]
    for s in range(SLOTS):
        src = pk_ref if s < KVH else pv_ref
        total = jnp.zeros((PROMPT, HD), jnp.bfloat16)
        for k in range(bank):
            hit = jnp.full((PROMPT, HD), task, jnp.int32) == me * bank + k
            total = jnp.where(hit, src[k, :, head_cols(s % KVH)], total)
        sel[s * PROMPT:(s + 1) * PROMPT, :] = total

    for i in (3, 1, 2):
        loads[i].wait()
    pl.semaphore_wait(barrier, n - 1 + n_dp - 1)

    def seg_copy(src_rank, dst_rank):
        return remote(seg_ref, segs.at[src_rank], seg_s.at[dst_rank], seg_r.at[src_rank], dp, dst_rank)

    half = SLOTS * PROMPT // 2

    def half_rows(side):
        return pl.ds(pl.multiple_of(side * half, half), half)

    def lane(h):
        return h * 2 + lo

    def swap_copy():
        return remote(sel.at[half_rows(1 - lo)], xa, sw_s.at[0], sw_r.at[0], dp, me + 1 - 2 * lo)

    def prs_copy(src_h, dst_h):
        return remote(chunk(mix, dst_h), prs.at[src_h], prs_s.at[dst_h], prs_r.at[src_h], dp, lane(dst_h))

    def pag_copy(src_h, dst_h):
        here = chunk(pp, lo * n_hi + src_h)
        return remote(here, here, pag_s.at[dst_h], pag_r.at[src_h], dp, lane(dst_h))

    def back_copy(side):
        here = pp.at[half_rows(side)]
        return remote(here, here, sw_s.at[1], sw_r.at[1], dp, me + 1 - 2 * lo)

    def z_copy(src, blk, j):
        return remote(src, kv.at[blk * 2 + lo, j], z_s.at[blk, j], z_r.at[blk, j], dp,
                      jnp.minimum(me + 2, n - 1 - (1 - lo)))

    def x_copy(src, blk, j, side):
        return remote(src, kv.at[blk * 2 + side, j], x_s.at[blk, j], x_r.at[blk, j], dp, me + 1 - 2 * lo)

    def w_copy():
        here = kv.at[1 - lo, 1]
        return remote(here, here, w_s.at[0], w_r.at[0], dp, jnp.minimum(me + 2, n - 1 - (1 - lo)))

    @pl.loop(1, n)
    def _(d):
        seg_copy(me, other(d, me, n)).start()

    swap_copy().start()
    own = (k_ref, v_ref)

    for j in range(2):
        @pl.when(hi + 1 < n_hi)
        def _():
            z_copy(own[j], hi, j).start()

        @pl.when(jnp.logical_or(lo == 0, hi == 0) if j else lo == 0)
        def _():
            x_copy(own[j], hi, j, lo).start()

    def queries(c):
        return jnp.concatenate([q_ref[:, head_cols(c * GROUP + g)] for g in range(GROUP)], axis=0)

    def grads(c):
        return jnp.concatenate([g_ref[:, head_cols(c * GROUP + g)] for g in range(GROUP)], axis=0)

    def wide(mask):
        return jnp.concatenate([mask] * GROUP, axis=1)

    loads[0].wait()
    q_seg = seg_ref[...]

    def column(row):
        return jnp.transpose(jnp.broadcast_to(row, (tok, tok)))

    def absorb(key_block, value_block, mask, first=False, heads=range(KVH)):
        mask = wide(mask)
        for c in heads:
            st = dot_nt(key_block[:, head_cols(c)], queries(c)) * scale
            st = jnp.where(mask, st, -jnp.inf)
            peak = jnp.max(st, axis=0, keepdims=True)
            if not first:
                old = m_ref[c]
                peak = jnp.maximum(old, peak)
                shrink = jnp.exp(old - peak)
            w = jnp.exp(st - peak)
            total = jnp.sum(w, axis=0, keepdims=True)
            acc = dot_tn(value_block[:, head_cols(c)], w.astype(jnp.bfloat16))
            if not first:
                total = total + l_ref[c] * shrink
                acc = acc + acc_ref[c] * shrink
            m_ref[c] = peak
            l_ref[c] = total
            acc_ref[c] = acc

    order = lax.broadcasted_iota(jnp.int32, (tok, tok), 0) <= lax.broadcasted_iota(jnp.int32, (tok, tok), 1)
    absorb(k_ref, v_ref, (column(q_seg) == jnp.broadcast_to(q_seg, (tok, tok))) & order, True)

    swap_copy().wait_recv()
    mix[...] = sel[half_rows(lo), :] + xa[...]

    @pl.loop(1, n_hi)
    def _(d):
        prs_copy(hi, other(d, hi, n_hi)).start()

    def spread_prompt():
        def prs_add(d, total):
            src = other(d, hi, n_hi)
            prs_copy(src, hi).wait_recv()
            return total + prs[src]

        first = mix[pl.ds(pl.multiple_of(hi * rows, rows), rows), :]
        pp[pl.ds(pl.multiple_of((lo * n_hi + hi) * rows, rows), rows), :] = lax.fori_loop(1, n_hi, prs_add, first)

        @pl.loop(1, n_hi)
        def _(d):
            pag_copy(hi, other(d, hi, n_hi)).start()

    def return_prompt():
        @pl.loop(1, n_hi)
        def _(d):
            pag_copy(other(d, hi, n_hi), hi).wait_recv()

        back_copy(lo).start()

    @pl.when(hi == 0)
    def _():
        x_copy(own[1], hi, 1, 1 - lo).wait_recv()

        @pl.when(hi + 1 < n_hi)
        def _():
            w_copy().start()
        spread_prompt()

    @pl.loop(1, n)
    def _(d):
        seg_copy(other(d, me, n), me).wait_recv()

    def absorb_rank(rank):
        mask = column(segs[rank]) == jnp.broadcast_to(q_seg, (tok, tok))
        absorb(kv.at[rank, 0], kv.at[rank, 1], mask)

    def absorb_crossed(blk):
        for j in range(2):
            x_copy(own[j], blk, j, 1 - lo).wait_recv()
        absorb_rank(blk * 2 + 1 - lo)

    @pl.loop(1, hi + 1)
    def _(s):
        blk = hi - s
        pl.when(jnp.logical_and(s == hi, hi >= 3))(return_prompt)
        for j in range(2):
            z_copy(own[j], blk, j).wait_recv()

            @pl.when(hi + 1 < n_hi)
            def _():
                z_copy(kv.at[blk * 2 + lo, j], blk, j).start()

            @pl.when(blk > 0 if j else blk >= 0)
            def _():
                x_copy(kv.at[blk * 2 + lo, j], blk, j, lo).start()

        @pl.when(jnp.logical_and(s == hi, hi + 1 < n_hi))
        def _():
            w_copy().wait_recv()
            w_copy().start()
        pl.when(s == jnp.minimum(hi, 2))(spread_prompt)
        absorb_rank(blk * 2 + lo)

        @pl.when(jnp.logical_or(s > 1, lo == 1))
        def _():
            absorb_crossed(blk + 1)

    pl.when(hi < 3)(return_prompt)
    back_copy(1 - lo).wait_recv()

    loads[6].wait()
    for c in range(KVH):
        pk = pp[c * PROMPT:(c + 1) * PROMPT, :]
        pv = pp[(KVH + c) * PROMPT:(KVH + c + 1) * PROMPT, :]
        r = dot_nt(pk, queries(c)) * scale
        old = m_ref[c]
        peak = jnp.maximum(old, jnp.max(r, axis=0, keepdims=True))
        shrink = jnp.exp(old - peak)
        w = jnp.exp(r - peak)
        m_ref[c] = peak
        l_ref[c] = jnp.sum(w, axis=0, keepdims=True) + l_ref[c] * shrink
        acc_ref[c] = dot_tn(pv, w.astype(jnp.bfloat16)) + acc_ref[c] * shrink
        r_ref[c] = r
        d_ref[c] = dot_nt(pv, grads(c))

    @pl.when(jnp.logical_and(hi > 0, hi + 1 == n_hi))
    def _():
        w_copy().wait_recv()

    crossed = jnp.logical_or(hi > 0, lo == 1)

    @pl.when(crossed)
    def _():
        near_ref[...] = column(segs[1 - lo])
        x_copy(own[0], 0, 0, 1 - lo).wait_recv()

    def grs_copy(src_rank, dst_rank):
        return remote(chunk(part, dst_rank), grs.at[src_rank], grs_s.at[dst_rank], grs_r.at[src_rank], dp, dst_rank)

    per_slot = n // SLOTS

    def send_slot(s):
        for i in range(per_slot):
            dst = s * per_slot + i

            @pl.when(me != dst)
            def _():
                grs_copy(me, dst).start()

    for c in range(KVH):
        @pl.when(crossed)
        def _():
            mask = near_ref[...] == jnp.broadcast_to(q_seg, (tok, tok))
            absorb(kv.at[1 - lo, 0], kv.at[1 - lo, 1], mask, heads=(c,))

        q = queries(c)
        g = grads(c)
        total = l_ref[c]
        att = jnp.transpose(acc_ref[c] / total).astype(jnp.bfloat16)
        for i in range(GROUP):
            att_ref[:, head_cols(c * GROUP + i)] = att[i * tok:(i + 1) * tok, :]
        delta = jnp.sum(jnp.transpose(g.astype(jnp.float32) * att.astype(jnp.float32)), axis=0, keepdims=True)
        probs = jnp.exp(r_ref[c] - (m_ref[c] + jnp.log(total)))
        score_grad = probs * (d_ref[c] - delta)
        vp = dot_nn(probs.astype(jnp.bfloat16), g)
        kp = dot_nn(score_grad.astype(jnp.bfloat16), q) * scale
        part[c * PROMPT:(c + 1) * PROMPT, :] = kp.astype(jnp.bfloat16)
        part[(KVH + c) * PROMPT:(KVH + c + 1) * PROMPT, :] = vp.astype(jnp.bfloat16)
        send_slot(c)
        send_slot(KVH + c)

    def grs_add(d, total):
        src = other(d, me, n)
        grs_copy(src, me).wait_recv()
        return total + grs[src].astype(jnp.float32)

    mine = pl.ds(pl.multiple_of(me * rows, rows), rows)
    gath[dp, mine, :] = lax.fori_loop(1, n, grs_add, part[mine, :].astype(jnp.float32)).astype(jnp.bfloat16)

    def piece(b, j):
        return gath.at[b, pl.ds(pl.multiple_of(j * rows, rows), rows)]

    def gag_copy(src_rank, dst_rank):
        return remote(piece(dp, src_rank), piece(dp, src_rank), gag_s.at[dst_rank], gag_r.at[src_rank], dp, dst_rank)

    def y_copy(src_h, dst_h, j):
        b = src_h * 2 + dl
        return remote(piece(b, j), piece(b, j), y_s.at[dst_h, j], y_r.at[src_h, j], dst_h * 2 + dl, me)

    def c_copy(h, side, j):
        b = h * 2 + side
        return remote(piece(b, j), piece(b, j), c_s.at[h, j], c_r.at[h, j], dh * 2 + 1 - dl, me)

    @pl.loop(1, n)
    def _(d):
        gag_copy(me, other(d, me, n)).start()

    def pass_on(j):
        @pl.loop(1, n_dh)
        def _(e):
            y_copy(dh, other(e, dh, n_dh), j).start()
        c_copy(dh, dl, j).start()

    pass_on(me)

    @pl.loop(1, n)
    def _(d):
        dst = other(d, me, n)
        seg_copy(me, dst).wait_send()
        grs_copy(me, dst).wait_send()

    swap_copy().wait_send()
    pl.when(hi + 1 < n_hi)(lambda: w_copy().wait_send())
    back_copy(lo).wait_send()

    @pl.loop(1, n_hi)
    def _(d):
        dst = other(d, hi, n_hi)
        prs_copy(hi, dst).wait_send()
        pag_copy(hi, dst).wait_send()

    for j in range(2):
        @pl.when(jnp.logical_or(lo == 0, hi == 0) if j else lo == 0)
        def _():
            x_copy(own[j], hi, j, lo).wait_send()

        @pl.loop(j, hi)
        def _(blk):
            x_copy(own[j], blk, j, lo).wait_send()

        @pl.when(hi + 1 < n_hi)
        def _():
            @pl.loop(0, hi + 1)
            def _(blk):
                z_copy(own[j], blk, j).wait_send()

    @pl.loop(1, n)
    def _(d):
        src = other(d, me, n)
        gag_copy(src, me).wait_recv()
        pass_on(src)

    @pl.loop(0, n)
    def _(d):
        src = other(d, me, n)

        @pl.loop(1, n_dh)
        def _(e):
            h = other(e, dh, n_dh)
            y_copy(h, dh, src).wait_recv()
            c_copy(h, dl, src).start()

    @pl.loop(0, n)
    def _(d):
        src = other(d, me, n)

        @pl.loop(0, n_dh)
        def _(h):
            c_copy(h, 1 - dl, src).wait_recv()

    @pl.loop(1, n)
    def _(d):
        gag_copy(me, other(d, me, n)).wait_send()

    @pl.loop(0, n)
    def _(j):
        @pl.loop(1, n_dh)
        def _(e):
            y_copy(dh, other(e, dh, n_dh), j).wait_send()

        @pl.loop(0, n_dh)
        def _(h):
            c_copy(h, dl, j).wait_send()


def finish(n_dp, task_ref, att_v, gath_v, att_out, kg_out, vg_out, kg_v, vg_v, out_s):
    bank = kg_v.shape[0]
    me = lax.axis_index("seq")
    stores = [pltpu.make_async_copy(att_v, att_out, out_s.at[2 * bank])]
    stores[0].start()
    for s in range(SLOTS):
        held, out = (kg_v, kg_out) if s < KVH else (vg_v, vg_out)
        for k in range(bank):
            total = jnp.zeros((PROMPT, HD), jnp.float32)
            for b in range(n_dp):
                hit = jnp.full((PROMPT, HD), task_ref[b], jnp.int32) == me * bank + k
                total = total + jnp.where(
                    hit, gath_v[b, s * PROMPT:(s + 1) * PROMPT, :].astype(jnp.float32), 0.0)
            held[k, :, head_cols(s % KVH)] = total
            if s % KVH == KVH - 1:
                stores.append(pltpu.make_async_copy(held.at[k], out.at[k], out_s.at[s // KVH * bank + k]))
                stores[-1].start()
    for store in stores:
        store.wait()


def shards(n, n_dp, queries, keys, values, segments, task_ids, prompt_keys, prompt_values, grad_out):
    tok = queries.shape[1]
    width = KVH * HD
    rows = SLOTS * PROMPT // n
    bank = prompt_keys.shape[0]
    bf16, f32 = jnp.bfloat16, jnp.float32
    dma = pltpu.SemaphoreType.DMA
    vmem = pl.BlockSpec(memory_space=pltpu.VMEM)
    operands = (queries[0], keys[0], values[0], segments, prompt_keys, prompt_values, grad_out[0])
    att, gath = pl.pallas_call(
        functools.partial(kernel, n, n_dp),
        out_shape=(
            pltpu.VMEM((tok, KVH * GROUP * HD), bf16),
            pltpu.VMEM((n_dp, SLOTS * PROMPT, HD), bf16),
        ),
        in_specs=[pl.BlockSpec(memory_space=pltpu.SMEM)] + [pl.BlockSpec(memory_space=pl.ANY)] * 7,
        out_specs=(vmem, vmem),
        scratch_shapes=[
            [pltpu.VMEM(a.shape, a.dtype) for a in operands],
            dma((7,)),
            pltpu.VMEM((n, 2, tok, width), bf16),
            pltpu.VMEM((n, 1, tok), jnp.int32),
            pltpu.VMEM((SLOTS * PROMPT, HD), bf16),
            pltpu.VMEM((tok, tok), jnp.int32),
            pltpu.VMEM((SLOTS * PROMPT // 2, HD), bf16),
            pltpu.VMEM((SLOTS * PROMPT // 2, HD), bf16),
            dma((1,)), dma((1,)), dma((2,)), dma((2,)),
            pltpu.VMEM((n // 2, rows, HD), bf16),
            pltpu.VMEM((SLOTS * PROMPT, HD), bf16),
            pltpu.VMEM((SLOTS * PROMPT, HD), bf16),
            pltpu.VMEM((n, rows, HD), bf16),
            pltpu.VMEM((KVH, 1, GROUP * tok), f32),
            pltpu.VMEM((KVH, 1, GROUP * tok), f32),
            pltpu.VMEM((KVH, HD, GROUP * tok), f32),
            pltpu.VMEM((KVH, PROMPT, GROUP * tok), f32),
            pltpu.VMEM((KVH, PROMPT, GROUP * tok), f32),
            dma((n,)), dma((n,)), dma((n // 2,)), dma((n // 2,)), dma((n // 2,)), dma((n // 2,)),
            dma((n // 2, 2)), dma((n // 2, 2)), dma((n // 2, 2)), dma((n // 2, 2)),
            dma((n,)), dma((n,)), dma((n,)), dma((n,)),
            dma((n_dp // 2, n)), dma((n_dp // 2, n)), dma((n_dp // 2, n)), dma((n_dp // 2, n)),
        ],
        compiler_params=pltpu.CompilerParams(collective_id=0, has_side_effects=True),
    )(task_ids, *operands)
    anyspace = pl.BlockSpec(memory_space=pl.ANY)
    att, kg, vg = pl.pallas_call(
        functools.partial(finish, n_dp),
        out_shape=(
            jax.ShapeDtypeStruct((tok, KVH * GROUP * HD), bf16),
            jax.ShapeDtypeStruct((bank, PROMPT, width), f32),
            jax.ShapeDtypeStruct((bank, PROMPT, width), f32),
        ),
        in_specs=[pl.BlockSpec(memory_space=pltpu.SMEM), vmem, vmem],
        out_specs=(anyspace, anyspace, anyspace),
        scratch_shapes=[
            pltpu.VMEM((bank, PROMPT, width), f32),
            pltpu.VMEM((bank, PROMPT, width), f32),
            dma((2 * bank + 1,)),
        ],
    )(task_ids, *[pltpu.with_memory_space_constraint(a, pltpu.VMEM) for a in (att, gath)])
    return att[None], kg, vg


def solution(mesh):
    n, n_dp = mesh.shape["seq"], mesh.shape["dp"]
    in_specs = (
        P("dp", "seq", None),
        P("dp", "seq", None),
        P("dp", "seq", None),
        P("dp", "seq"),
        P(),
        P("seq", None, None),
        P("seq", None, None),
        P("dp", "seq", None),
    )
    out_specs = (P("dp", "seq", None), P("seq", None, None), P("seq", None, None))
    return jax.shard_map(
        functools.partial(shards, n, n_dp), mesh=mesh, in_specs=in_specs, out_specs=out_specs, check_vma=False
    )
```
